256 devices in a mesh: dp: 16 (over y_hi, z), tensor: 16 (over y_lo, x, core).
Axes of the slice: x: 4, y: 4 (y_hi: 2, y_lo: 2; y = y_hi * 2 + y_lo), z: 8, core: 2. Of those that a mesh axis runs over, the one named last changes fastest.
Arguments:
- q_nope: bfloat16 [64, 2, 128, 128], P('dp', None, 'tensor'), parts along dimension 0, may hold values from -6 to 6
- q_rope: bfloat16 [64, 2, 128, 64], P('dp', None, 'tensor'), parts along dimension 0, may hold values from -8 to 8
- w_uk: bfloat16 [128, 128, 512], P('tensor'), may hold values from -0.5 to 0.5
- w_uv: bfloat16 [128, 512, 128], P('tensor'), may hold values from -0.25 to 0.25
- cache_latent: bfloat16 [64, 32768, 512], P('dp', 'tensor'), parts along dimension 0, may hold values from -4 to 4
- cache_rope: bfloat16 [64, 64, 32768], P('dp', None, 'tensor'), parts along dimension 0, may hold values from -14 to 14
- scale_pool: float32 [5, 16384], P(None, ('dp', 'tensor')), parts along dimension 1, may hold values from 0.3 to 3
- block_index: int32 [64, 256], P('dp', 'tensor'), parts along dimension 0, may hold values from 0 to 1023, as said below
- lengths: int32 [64], P('dp'), parts along dimension 0, may hold values from 8192 to 32768, as said below
Outputs:
- head_outputs: bfloat16 [64, 2, 128, 128], P('dp', None, 'tensor'), parts along dimension 0
The draws below stay inside these ranges and needn't reach their ends.
There are 16 independent parts, one for each index of `dp`. The reference program is written for one: setup_inputs(seed, part) draws one part's arguments, and reference() takes and returns one part's arrays. A program takes and returns all parts, laid end to end along the dimension named above; an argument that names none is the same for every part. Nothing has to cross between parts.
Inputs may be any that keep to these rules, and one draw needn't show every extreme that they name: `block_index`: every column of the scale table is named by exactly one cache block of the group. `lengths`: in a group of two or more requests, one request is shorter than 16384 and the others are at least 16384 long.
All inputs are finite; a program needn't handle non-finite values.
Results may differ from the reference program's by a relative error of at most 0.012.
Values may be sent and summed in bfloat16 or wider, within the bound.
A program may use at most 128 MiB of HBM per device.

```python
import math
import jax
import jax.numpy as jnp
from jax import lax

REQS = 4
QTOK = 2
HEADS = 128
NOPE = 128
ROPE = 64
LATENT = 512
VDIM = 128
GROUPS = 5
CTX = 32768
NBLK = 256
POOL = 1024


def shared(key):
    base_key = jax.random.fold_in(key, 9173)
    key_d = jax.random.fold_in(base_key, 3)
    pool_order = jax.random.permutation(key_d, POOL).astype(jnp.int32).reshape(REQS, NBLK)
    return pool_order


def draw_lengths(key, part):
    own_key = jax.random.fold_in(key, 57)
    key_a, key_b, key_c = jax.random.split(own_key, 3)
    short_ones = jax.random.randint(key_a, (REQS,), CTX // 4, CTX // 2)
    long_ones = jax.random.randint(key_b, (REQS,), CTX // 2, CTX + 1)
    short_pick = jax.random.randint(key_c, (), 0, REQS)
    which = jnp.arange(REQS, dtype=jnp.int32) == short_pick
    return jnp.where(which, short_ones, long_ones).astype(jnp.int32)


def draw_block_index(key, part):
    pool_order = shared(key)
    return pool_order


def draw_scale_pool(key, part):
    own_key = jax.random.fold_in(key, 31)
    logs_drawn = jax.random.uniform(own_key, (GROUPS, POOL), jnp.float32, math.log(0.3), math.log(3.0))
    values = jnp.exp(logs_drawn)
    return values.astype(jnp.float32)


def draw_q_rope(key, part):
    full_shape = (REQS, QTOK, HEADS, ROPE)
    own_key = jax.random.fold_in(key, 11)
    values = jnp.clip(jax.random.normal(own_key, full_shape, jnp.float32), -4.0, 4.0)
    return values.astype(jnp.bfloat16)


def draw_cache_latent(key, part):
    full_shape = (REQS, CTX, LATENT)
    own_key = jax.random.fold_in(key, 21)
    values = jnp.clip(jax.random.normal(own_key, full_shape, jnp.float32), -4.0, 4.0)
    return values.astype(jnp.bfloat16)


def draw_cache_rope(key, part):
    full_shape = (REQS, ROPE, CTX)
    own_key = jax.random.fold_in(key, 41)
    values = jnp.clip(jax.random.normal(own_key, full_shape, jnp.float32), -4.0, 4.0)
    return values.astype(jnp.bfloat16)


def shard_levels(key, extent, pieces, smallest, high):
    loudness = 1.0
    for axis_at, parts in pieces:
        draws = jax.random.uniform(jax.random.fold_in(jax.random.fold_in(key, 6), axis_at), (parts,), jnp.float32, smallest / len(pieces), high / len(pieces))
        loudness = loudness * jnp.repeat(jnp.exp(draws), extent[axis_at] // parts).reshape((-1,) + (1,) * (len(extent) - 1 - axis_at))
    return loudness


def scatter_about(key, extent, deviation, bound, cuts=(), kind=jnp.bfloat16):
    drawn = jax.random.normal(key, extent, jnp.float32) * deviation
    if len(cuts) > 0:
        drawn = shard_levels(key, extent, cuts, -0.22, 0.18) * drawn
    return jnp.clip(drawn, min=-bound, max=bound).astype(kind)


def setup_inputs(seed: int = 0, part: int = 0) -> dict:
    seeds = jax.random.split(jax.random.key(seed), 10)
    own_keys = jax.random.split(jax.random.fold_in(seeds[9], part), 10)
    q_nope = scatter_about(own_keys[0], (REQS, QTOK, HEADS, NOPE), 1.0, 6.0, ((2, 16),))
    q_rope = draw_q_rope(jax.random.fold_in(jax.random.fold_in(seeds[9], part), 71), part)
    w_uk = scatter_about(seeds[2], (HEADS, NOPE, LATENT), NOPE ** -0.5, 0.5, ((0, 16),))
    w_uv = scatter_about(seeds[3], (HEADS, LATENT, VDIM), LATENT ** -0.5, 0.25, ((0, 16),))
    cache_latent = draw_cache_latent(jax.random.fold_in(jax.random.fold_in(seeds[9], part), 71), part)
    cache_rope = draw_cache_rope(jax.random.fold_in(jax.random.fold_in(seeds[9], part), 71), part)
    scale_pool = draw_scale_pool(jax.random.fold_in(jax.random.fold_in(seeds[9], part), 71), part)
    block_index = draw_block_index(jax.random.fold_in(jax.random.fold_in(seeds[9], part), 71), part)
    lengths = draw_lengths(jax.random.fold_in(jax.random.fold_in(seeds[9], part), 71), part)
    return dict(q_nope=q_nope, q_rope=q_rope, w_uk=w_uk, w_uv=w_uv, cache_latent=cache_latent, cache_rope=cache_rope, scale_pool=scale_pool, block_index=block_index, lengths=lengths)


masked_score = -1e30


def one_request(operands):
    query_latent, query_rope, latent_codes, rope_codes, scales, length = operands
    blocks = scales.shape[1]
    groups = scales.shape[0]
    block_width = latent_codes.shape[0] // blocks
    latent_scale = jnp.transpose(scales[:groups - 1])[:, None, :, None]
    latent_full = (latent_codes.astype(jnp.float32).reshape(blocks, block_width, groups - 1, -1) * latent_scale).astype(jnp.bfloat16).reshape(latent_codes.shape)
    rope_scale = scales[groups - 1][None, :, None]
    rope_full = (rope_codes.astype(jnp.float32).reshape(rope_codes.shape[0], blocks, block_width) * rope_scale).astype(jnp.bfloat16).reshape(rope_codes.shape)
    new_tokens = query_latent.shape[0]
    head_count = query_latent.shape[1]
    latent_rows = query_latent.reshape(new_tokens * head_count, -1)
    rope_rows = query_rope.reshape(new_tokens * head_count, -1)
    scores = jnp.dot(latent_rows, latent_full.T, preferred_element_type=jnp.float32) + jnp.dot(rope_rows, rope_full, preferred_element_type=jnp.float32)
    scores = scores * ((NOPE + ROPE) ** -0.5)
    positions = jnp.arange(CTX, dtype=jnp.int32)
    limits = length - QTOK + jnp.arange(QTOK, dtype=jnp.int32)
    allowed = positions[None, :] <= limits[:, None]
    allowed = jnp.repeat(allowed, head_count, axis=0)
    scores = jnp.where(allowed, scores, masked_score)
    peak_score = jnp.max(scores, axis=1, keepdims=True)
    weights = jnp.exp(scores - peak_score)
    totals = jnp.sum(weights, axis=1, keepdims=True)
    mixture = jnp.dot(weights.astype(jnp.bfloat16), latent_full, preferred_element_type=jnp.float32)
    attended = (mixture / totals).astype(jnp.bfloat16)
    return attended.reshape(new_tokens, head_count, -1)


def reference(q_nope, q_rope, w_uk, w_uv, cache_latent, cache_rope, scale_pool, block_index, lengths):
    query_latent = jnp.einsum("rthn,hnc->rthc", q_nope.astype(jnp.float32), w_uk.astype(jnp.float32)).astype(jnp.bfloat16)
    block_scale = jnp.take(scale_pool, block_index, axis=1)
    per_request = jnp.moveaxis(block_scale, 1, 0)
    attended = lax.map(one_request, (query_latent, q_rope, cache_latent, cache_rope, per_request, lengths))
    head_outputs = jnp.einsum("rthc,hcv->rthv", attended.astype(jnp.float32), w_uv.astype(jnp.float32))
    return head_outputs.astype(jnp.bfloat16)
```

```python
import functools
import math

import jax
import jax.numpy as jnp
from jax import lax
from jax.experimental import pallas as pl
from jax.experimental.pallas import tpu as pltpu
from jax.sharding import PartitionSpec as P

MESH = pl.DeviceIdType.MESH
R, T, H = 4, 2, 8
ROWS, LAT, ROPE, WIDE = 256, 512, 64, 640
SPAN, BLOCKS = 2048, 16
X, CHIPS = 4, 8
FACTOR = (128 + 64) ** -0.5 * math.log2(math.e)
MASKED = -1e30
F32, BF16 = jnp.float32, jnp.bfloat16


def parts_of(value, count):
    parts = []
    for _ in range(count):
        part = value.astype(BF16).astype(F32)
        parts.append(part)
        value = value - part
    return parts


def stats_tile(peak, total):
    lane = lax.broadcasted_iota(jnp.int32, (peak.shape[0], 128), 1)
    tile = jnp.zeros((peak.shape[0], 128), F32)
    for at, part in enumerate(parts_of(peak, 3) + parts_of(total, 2)):
        tile = jnp.where(lane == at, part, tile)
    return tile.astype(BF16)


def stats_of(tile):
    tile = tile.astype(F32)
    return tile[:, 0:1] + tile[:, 1:2] + tile[:, 2:3], tile[:, 3:4] + tile[:, 4:5]


def kernel(
    q_nope, q_rope, w_uk, w_uv, latent, rope, pool, index, lengths, out,
    nope_v, qrope_v, uk_v, uv_v, lat, rop, table, table_s, index_s, length_s,
    qf, flat, queries, scores, weights, mixed, peaks, sums, out_a, in_a, out_b, in_b, att, res, res_b,
    load_sem, table_sem, table_send, table_recv, q_send, q_recv, f_send, f_recv,
    a_send, a_recv, b_send, b_recv, out_sem,
):
    me = lax.axis_index("tensor")
    core = lax.rem(me, 2)
    chip = me // 2
    row, column = chip // X, lax.rem(chip, X)
    partner = me + 1 - 2 * core

    def peer(j, sign):
        dy, dx = j // X, j % X
        other = lax.rem(row + dy, 2) * X + lax.rem(column + (dx if sign > 0 else X - dx), X)
        return other * 2 + core

    def remote(src, dst, send, recv, to):
        return pltpu.make_async_remote_copy(
            src_ref=src, dst_ref=dst, send_sem=send, recv_sem=recv,
            device_id={"tensor": to}, device_id_type=MESH,
        )

    barrier = pltpu.get_barrier_semaphore()
    for step in range(1, 16):
        pl.semaphore_signal(
            barrier, inc=1, device_id={"tensor": lax.rem(me + step, 16)}, device_id_type=MESH
        )

    small = [
        pltpu.make_async_copy(w_uk, uk_v, load_sem.at[0]),
        pltpu.make_async_copy(q_nope, nope_v, load_sem.at[1]),
        pltpu.make_async_copy(q_rope, qrope_v, load_sem.at[2]),
        pltpu.make_async_copy(pool, table.at[0], load_sem.at[3]),
        pltpu.make_async_copy(index, index_s, load_sem.at[4]),
        pltpu.make_async_copy(lengths, length_s, load_sem.at[5]),
    ]
    big = []
    for r in range(R):
        big.append(pltpu.make_async_copy(latent.at[r], lat.at[r], load_sem.at[6 + r]))
        big.append(pltpu.make_async_copy(rope.at[r], rop.at[r], load_sem.at[10 + r]))
    late = pltpu.make_async_copy(w_uv, uv_v, load_sem.at[14])
    for copy in small + big + [late]:
        copy.start()
    for copy in small:
        copy.wait()

    qf[...] = nope_v[...].astype(F32).reshape(R * T * H, 128)
    for h in range(H):
        rows = qf[pl.ds(h, R * T, stride=H), :].astype(BF16)
        got = jnp.dot(rows, uk_v[h], preferred_element_type=F32)
        for g in range(4):
            flat[g, pl.ds(h, R * T, stride=H), :] = got[:, 128 * g : 128 * (g + 1)]
    for r in range(R):
        for g in range(4):
            queries[r, 0:16, 128 * g : 128 * (g + 1)] = flat[g, 16 * r : 16 * (r + 1), :].astype(BF16)
        turned = qrope_v[r].astype(F32).reshape(16, ROPE)
        queries[r, 0:16, LAT:WIDE] = jnp.concatenate([turned, jnp.zeros((16, 64), F32)], axis=1).astype(BF16)

    pl.semaphore_wait(barrier, 15)

    table_copies = []
    for step in range(1, 16):
        table_copies.append(
            remote(table.at[0], table.at[step], table_send.at[step - 1], table_recv.at[step - 1],
                   lax.rem(me + 16 - step, 16))
        )
    for copy in table_copies:
        copy.start()
    q_copies = []
    for r in range(R):
        q_copies.append([
            remote(queries.at[r, pl.ds(0, 16)], queries.at[r, pl.ds(16 * j, 16)],
                   q_send.at[r, j - 1], q_recv.at[r, j - 1], peer(j, -1))
            for j in range(1, CHIPS)
        ])
        for copy in q_copies[r]:
            copy.start()
    f_copies = [
        remote(queries.at[r, pl.ds(0, 128)], queries.at[r, pl.ds(128, 128)],
               f_send.at[r], f_recv.at[r], partner)
        for r in range(R)
    ]
    a_copies = [
        remote(out_a.at[r], in_a.at[r], a_send.at[r], a_recv.at[r], partner) for r in range(R)
    ]
    b_copies = [
        [
            remote(out_b.at[r, pl.ds(16 * j, 16)], in_b.at[r, pl.ds(16 * j, 16)],
                   b_send.at[r, j - 1], b_recv.at[r, j - 1], peer(j, 1))
            for j in range(1, CHIPS)
        ]
        for r in range(R)
    ]

    for copy in table_copies:
        copy.wait_recv()
    to_scalar = pltpu.make_async_copy(table, table_s, table_sem)
    to_scalar.start()
    to_scalar.wait()

    def scale(r):
        big[2 * r].wait()
        big[2 * r + 1].wait()

        def one(b, carry):
            at = index_s[r, b]
            slot = lax.rem(at // 64 + 16 - me, 16)
            col = lax.rem(at, 64)
            rows = pl.ds(pl.multiple_of(b * 128, 128), 128)
            for g in range(4):
                lat[r, rows, 128 * g : 128 * (g + 1)] = (
                    lat[r, rows, 128 * g : 128 * (g + 1)].astype(F32) * table_s[slot, g, col]
                ).astype(BF16)
            rop[r, :, rows] = (rop[r, :, rows].astype(F32) * table_s[slot, 4, col]).astype(BF16)
            return carry

        lax.fori_loop(0, BLOCKS, one, 0)

    WIDTH = 512
    CHUNKS = SPAN // WIDTH

    def attend(r):
        length = length_s[r]

        def score(n, top):
            cols = pl.ds(pl.multiple_of(n * WIDTH, WIDTH), WIDTH)
            got = lax.dot_general(
                queries[r, :, 0:LAT], lat[r, cols, :], (((1,), (1,)), ((), ())),
                preferred_element_type=F32,
            ) + jnp.dot(queries[r, :, LAT : LAT + ROPE], rop[r, :, cols], preferred_element_type=F32)
            place = lax.broadcasted_iota(jnp.int32, (1, T, 8, WIDTH), 3) + (me * SPAN + n * WIDTH)
            limit = length - T + lax.broadcasted_iota(jnp.int32, (1, T, 8, WIDTH), 1)
            got = jnp.where(place <= limit, got.reshape(16, T, 8, WIDTH), MASKED).reshape(ROWS, WIDTH)
            scores[:, cols] = got
            for g in range(WIDTH // 128):
                top = jnp.maximum(top, got[:, 128 * g : 128 * (g + 1)])
            return top

        top = lax.fori_loop(0, CHUNKS, score, jnp.full((ROWS, 128), -3e38, F32))
        peak = jnp.max(top, axis=1, keepdims=True)

        def weigh(n, total):
            cols = pl.ds(pl.multiple_of(n * WIDTH, WIDTH), WIDTH)
            got = jnp.exp2((scores[:, cols] - peak) * FACTOR)
            weights[:, cols] = got.astype(BF16)
            for g in range(WIDTH // 128):
                total = total + got[:, 128 * g : 128 * (g + 1)]
            return total

        total = lax.fori_loop(0, CHUNKS, weigh, jnp.zeros((ROWS, 128), F32))
        total = jnp.sum(total, axis=1, keepdims=True)
        got = jnp.dot(weights[...], lat[r], preferred_element_type=F32)
        out_a[r, :, 0:LAT] = got[128:].astype(BF16)
        out_a[r, :, LAT:WIDE] = stats_tile(peak[128:], total[128:])
        a_copies[r].start()
        mixed[r] = got[:128]
        peaks[r] = jnp.broadcast_to(peak[:128], (128, 128))
        sums[r] = jnp.broadcast_to(total[:128], (128, 128))

    def combine(r):
        a_copies[r].wait_recv()
        peak_0, total_0 = peaks[r, :, 0:1], sums[r, :, 0:1]
        peak_1, total_1 = stats_of(in_a[r, :, LAT:WIDE])
        peak = jnp.maximum(peak_0, peak_1)
        gain_0 = jnp.exp2((peak_0 - peak) * FACTOR)
        gain_1 = jnp.exp2((peak_1 - peak) * FACTOR)
        out_b[r, :, 0:LAT] = (mixed[r] * gain_0 + in_a[r, :, 0:LAT].astype(F32) * gain_1).astype(BF16)
        out_b[r, :, LAT:WIDE] = stats_tile(peak, total_0 * gain_0 + total_1 * gain_1)
        for copy in b_copies[r]:
            copy.start()

    def finish(r):
        for copy in b_copies[r]:
            copy.wait_recv()
        found = [stats_of(out_b[r, 0:16, LAT:WIDE])] + [
            stats_of(in_b[r, 16 * j : 16 * (j + 1), LAT:WIDE]) for j in range(1, CHIPS)
        ]
        peak = functools.reduce(jnp.maximum, [p for p, _ in found])
        total = jnp.zeros((16, 1), F32)
        summed = jnp.zeros((16, LAT), F32)
        for j, (p, t) in enumerate(found):
            gain = jnp.exp2((p - peak) * FACTOR)
            total = total + t * gain
            block = out_b[r, 0:16, 0:LAT] if j == 0 else in_b[r, 16 * j : 16 * (j + 1), 0:LAT]
            summed = summed + block.astype(F32) * gain
        attended = summed / total
        for g in range(4):
            att[g, 16 * r : 16 * (r + 1), :] = attended[:, 128 * g : 128 * (g + 1)]

    for r in range(R):
        for copy in q_copies[r]:
            copy.wait_recv()
        f_copies[r].start()
        scale(r)
        f_copies[r].wait_recv()
        attend(r)
        if r >= 1:
            combine(r - 1)
    combine(R - 1)
    for r in range(R):
        finish(r)

    late.wait()
    for h in range(H):
        rows = jnp.concatenate(
            [att[g, pl.ds(h, R * T, stride=H), :] for g in range(4)], axis=1
        ).astype(BF16)
        res[pl.ds(h, R * T, stride=H), :] = jnp.dot(rows, uv_v[h], preferred_element_type=F32)
    res_b[...] = res[...].reshape(R, T, H, 128).astype(BF16)
    done = pltpu.make_async_copy(res_b, out, out_sem)
    done.start()

    for copy in table_copies:
        copy.wait_send()
    for r in range(R):
        for copy in q_copies[r] + b_copies[r] + [f_copies[r], a_copies[r]]:
            copy.wait_send()
    done.wait()


def local(*args):
    dma = pltpu.SemaphoreType.DMA
    return pl.pallas_call(
        kernel,
        out_shape=jax.ShapeDtypeStruct((R, T, H, 128), BF16),
        in_specs=[pl.BlockSpec(memory_space=pl.ANY)] * 9,
        out_specs=pl.BlockSpec(memory_space=pl.ANY),
        scratch_shapes=[
            pltpu.VMEM((R, T, H, 128), BF16),
            pltpu.VMEM((R, T, H, ROPE), BF16),
            pltpu.VMEM((H, 128, LAT), BF16),
            pltpu.VMEM((H, LAT, 128), BF16),
            pltpu.VMEM((R, SPAN, LAT), BF16),
            pltpu.VMEM((R, ROPE, SPAN), BF16),
            pltpu.VMEM((16, 5, 64), F32),
            pltpu.SMEM((16, 5, 64), F32),
            pltpu.SMEM((R, BLOCKS), jnp.int32),
            pltpu.SMEM((R,), jnp.int32),
            pltpu.VMEM((R * T * H, 128), F32),
            pltpu.VMEM((4, R * T * H, 128), F32),
            pltpu.VMEM((R, ROWS, WIDE), BF16),
            pltpu.VMEM((ROWS, SPAN), F32),
            pltpu.VMEM((ROWS, SPAN), BF16),
            pltpu.VMEM((R, 128, LAT), F32),
            pltpu.VMEM((R, 128, 128), F32),
            pltpu.VMEM((R, 128, 128), F32),
            pltpu.VMEM((R, 128, WIDE), BF16),
            pltpu.VMEM((R, 128, WIDE), BF16),
            pltpu.VMEM((R, 128, WIDE), BF16),
            pltpu.VMEM((R, 128, WIDE), BF16),
            pltpu.VMEM((4, R * T * H, 128), F32),
            pltpu.VMEM((R * T * H, 128), F32),
            pltpu.VMEM((R, T, H, 128), BF16),
            dma((15,)),
            dma(()),
            dma((15,)),
            dma((15,)),
            dma((R, 7)),
            dma((R, 7)),
            dma((R,)),
            dma((R,)),
            dma((R,)),
            dma((R,)),
            dma((R, 7)),
            dma((R, 7)),
            dma(()),
        ],
        compiler_params=pltpu.CompilerParams(collective_id=0, has_side_effects=True),
        name="decode",
    )(*args)


def solution(mesh):
    placed = (
        P("dp", None, "tensor", None),
        P("dp", None, "tensor", None),
        P("tensor", None, None),
        P("tensor", None, None),
        P("dp", "tensor", None),
        P("dp", None, "tensor"),
        P(None, ("dp", "tensor")),
        P("dp", "tensor"),
        P("dp"),
    )
    return jax.shard_map(
        local, mesh=mesh, in_specs=placed, out_specs=P("dp", None, "tensor", None), check_vma=False
    )
```

```python
import functools
import math

import jax
import jax.numpy as jnp
from jax import lax
from jax.experimental import pallas as pl
from jax.experimental.pallas import tpu as pltpu
from jax.sharding import PartitionSpec as P

MESH = pl.DeviceIdType.MESH
R, T, H = 4, 2, 8
ROWS, LAT, ROPE, WIDE = 256, 512, 64, 640
SPAN, BLOCKS = 2048, 16
X, CHIPS = 4, 8
FACTOR = (128 + 64) ** -0.5 * math.log2(math.e)
MASKED = -1e30
UNROLL = 4
SCALE_UNROLL = 4
F32, BF16 = jnp.float32, jnp.bfloat16


ORDER = (6, 2, 5, 7, 1, 3, 4)
WIDTH = 512
CHUNKS = SPAN // WIDTH


def parts_of(value, count):
    parts = []
    for _ in range(count):
        part = value.astype(BF16).astype(F32)
        parts.append(part)
        value = value - part
    return parts


def stats_tile(peak, total):
    lane = lax.broadcasted_iota(jnp.int32, peak.shape, 1)
    tile = jnp.zeros(peak.shape, F32)
    for at, part in enumerate(parts_of(peak, 3) + parts_of(total, 2)):
        tile = jnp.where(lane == at, part, tile)
    return tile.astype(BF16)


def stats_of(tile):
    tile = tile.astype(F32)
    return tile[:, 0:1] + tile[:, 1:2] + tile[:, 2:3], tile[:, 3:4] + tile[:, 4:5]


def wide(tile):
    return jnp.concatenate([tile] * 4, axis=1)


def kernel(
    q_nope, q_rope, w_uk, w_uv, latent, rope, pool, index, lengths, out,
    nope_v, qrope_v, uk_v, uv_v, lat, rop, pool_v, table, index_s, length_s,
    qf, flat, queries, scores, weights, mixed, out_s, in_s, gains,
    out_a, in_a, out_b, in_b, out_t, in_t, att, res,
    load_sem, lat_sem, table_send, table_recv, q_send, q_recv, f_send, f_recv,
    s_send, s_recv, a_send, a_recv, t_send, t_recv, b_send, b_recv,
):
    me = lax.axis_index("tensor")
    core = lax.rem(me, 2)
    chip = me // 2
    row, column = chip // X, lax.rem(chip, X)
    partner = me + 1 - 2 * core

    def peer(j, sign):
        dy, dx = j // X, j % X
        other = lax.rem(row + dy, 2) * X + lax.rem(column + (dx if sign > 0 else X - dx), X)
        return other * 2 + core

    def remote(src, dst, send, recv, to):
        return pltpu.make_async_remote_copy(
            src_ref=src, dst_ref=dst, send_sem=send, recv_sem=recv,
            device_id={"tensor": to}, device_id_type=MESH,
        )

    barrier = pltpu.get_barrier_semaphore()
    for step in range(1, 16):
        pl.semaphore_signal(
            barrier, inc=1, device_id={"tensor": lax.rem(me + step, 16)}, device_id_type=MESH
        )

    small = [
        pltpu.make_async_copy(w_uk, uk_v, load_sem.at[0]),
        pltpu.make_async_copy(q_nope, nope_v, load_sem.at[1]),
        pltpu.make_async_copy(q_rope, qrope_v, load_sem.at[2]),
        pltpu.make_async_copy(pool, pool_v, load_sem.at[3]),
        pltpu.make_async_copy(index, index_s, load_sem.at[4]),
        pltpu.make_async_copy(lengths, length_s, load_sem.at[5]),
    ]
    big = []
    for r in range(R):
        big.append(pltpu.make_async_copy(latent.at[r], lat.at[r], lat_sem.at[r, 0]))
        big.append(pltpu.make_async_copy(rope.at[r], rop.at[r], lat_sem.at[r, 1]))
    late = pltpu.make_async_copy(w_uv, uv_v, load_sem.at[6])
    for copy in small:
        copy.start()
    with jax.named_scope("waitsmall"):
        for copy in small:
            copy.wait()
    own_table = pltpu.make_async_copy(pool_v, table.at[0], load_sem.at[7])
    for copy in [own_table] + big + [late]:
        copy.start()
    qf[...] = nope_v[...].astype(F32).reshape(R * T * H, 128)
    for h in range(H):
        rows = qf[pl.ds(h, R * T, stride=H), :].astype(BF16)
        got = jnp.dot(rows, uk_v[h], preferred_element_type=F32)
        for g in range(4):
            flat[g, pl.ds(h, R * T, stride=H), :] = got[:, 128 * g : 128 * (g + 1)]
    for r in range(R):
        for g in range(4):
            queries[r, 0:16, 128 * g : 128 * (g + 1)] = flat[g, 16 * r : 16 * (r + 1), :].astype(BF16)
        turned = qrope_v[r].astype(F32).reshape(16, ROPE)
        queries[r, 0:16, LAT:WIDE] = jnp.concatenate([turned, jnp.zeros((16, 64), F32)], axis=1).astype(BF16)

    with jax.named_scope("barrier"):
        pl.semaphore_wait(barrier, 15)
    table_copies = [
        remote(pool_v, table.at[step], table_send, table_recv, lax.rem(me + 16 - step, 16))
        for step in (8, 7, 9, 4, 5, 12, 11, 13, 3, 6, 10, 2, 14, 1, 15)
    ]
    for copy in table_copies:
        copy.start()

    q_copies = [
        [
            remote(queries.at[r, pl.ds(0, 16)], queries.at[r, pl.ds(16 * j, 16)],
                   q_send, q_recv.at[r], peer(j, -1))
            for j in ORDER
        ]
        for r in range(R)
    ]
    for r in range(R):
        for copy in q_copies[r]:
            copy.start()
    f_copies = [
        remote(queries.at[r, pl.ds(0, 128)], queries.at[r, pl.ds(128, 128)],
               f_send.at[r], f_recv.at[r], partner)
        for r in range(R)
    ]
    s_copies = [
        remote(out_s.at[r], in_s.at[r], s_send.at[r], s_recv.at[r], partner) for r in range(R)
    ]
    a_copies = [
        remote(out_a.at[r], in_a.at[r], a_send.at[r], a_recv.at[r], partner) for r in range(R)
    ]
    t_copies = [
        [
            remote(out_t.at[r, pl.ds(16 * j, 16)], in_t.at[r, pl.ds(16 * j, 16)],
                   t_send.at[r], t_recv.at[r], peer(j, 1))
            for j in ORDER
        ]
        for r in range(R)
    ]
    b_copies = [
        [
            remote(out_b.at[r, pl.ds(16 * j, 16)], in_b.at[r, pl.ds(16 * j, 16)],
                   b_send.at[r], b_recv.at[r], peer(j, 1))
            for j in ORDER
        ]
        for r in range(R)
    ]

    def seven(ref, send, recv):
        return remote(ref.at[pl.ds(16, 112)], ref.at[pl.ds(16, 112)], send, recv, partner)

    def forward(r):
        seven(queries.at[r], q_send, q_recv.at[r]).wait_recv()
        f_copies[r].start()

    with jax.named_scope("waittable"):
        remote(table.at[pl.ds(1, 15)], table.at[pl.ds(1, 15)], table_send, table_recv, partner).wait_recv()
        own_table.wait()

    def scale_block(r, b):
        at = index_s[r, b]
        slot = lax.rem(at // 64 + 16 - me, 16)
        col = lax.rem(at, 64)
        rows = pl.ds(pl.multiple_of(b * 128, 128), 128)
        for g in range(4):
            lat[r, rows, 128 * g : 128 * (g + 1)] = (
                lat[r, rows, 128 * g : 128 * (g + 1)].astype(F32) * table[slot, g, col]
            ).astype(BF16)
        rop[r, :, rows] = (rop[r, :, rows].astype(F32) * table[slot, 4, col]).astype(BF16)

    def loaded(r):
        big[2 * r].wait()
        big[2 * r + 1].wait()

    def scale(r):
        loaded(r)

        def one(b, carry):
            scale_block(r, b)
            return carry

        lax.fori_loop(0, BLOCKS, one, 0, unroll=SCALE_UNROLL)

    def score(r, n, top):
        cols = pl.ds(pl.multiple_of(n * WIDTH, WIDTH), WIDTH)
        got = lax.dot_general(
            queries[r, :, 0:LAT], lat[r, cols, :], (((1,), (1,)), ((), ())),
            preferred_element_type=F32,
        ) + jnp.dot(queries[r, :, LAT : LAT + ROPE], rop[r, :, cols], preferred_element_type=F32)
        place = lax.broadcasted_iota(jnp.int32, (1, T, 8, WIDTH), 3) + (me * SPAN + n * WIDTH)
        limit = length_s[r] - T + lax.broadcasted_iota(jnp.int32, (1, T, 8, WIDTH), 1)
        got = jnp.where(place <= limit, got.reshape(16, T, 8, WIDTH), MASKED).reshape(ROWS, WIDTH)
        scores[r % 2, :, cols] = got
        for g in range(WIDTH // 128):
            top = jnp.maximum(top, got[:, 128 * g : 128 * (g + 1)])
        return top

    def weigh(r, n, peak, total):
        cols = pl.ds(pl.multiple_of(n * WIDTH, WIDTH), WIDTH)
        got = jnp.exp2((scores[r % 2, :, cols] - peak) * FACTOR)
        weights[:, cols] = got.astype(BF16)
        for g in range(WIDTH // 128):
            total = total + got[:, 128 * g : 128 * (g + 1)]
        return total

    def both(r, peak, beside=None):
        top, total = jnp.full((ROWS, 128), -3e38, F32), jnp.zeros((ROWS, 128), F32)

        def one(n, carry):
            top, total = carry
            if r < R:
                top = score(r, n, top)
            if r > 0:
                total = weigh(r - 1, n, peak, total)
            if beside is not None:
                for b in range(BLOCKS // CHUNKS):
                    scale_block(beside, n * (BLOCKS // CHUNKS) + b)
            return top, total

        top, total = lax.fori_loop(0, CHUNKS, one, (top, total), unroll=UNROLL)
        if r < R:
            top = jnp.max(top, axis=1, keepdims=True)
        if r > 0:
            total = jnp.sum(total, axis=1, keepdims=True)
        return top, total

    def mix(r, peak, total):
        peak_w = jnp.broadcast_to(peak, (ROWS, 128))
        total_w = jnp.broadcast_to(total, (ROWS, 128))
        out_s[r, :, 0:128] = peak_w[128:]
        out_s[r, :, 128:256] = total_w[128:]
        s_copies[r].start()
        gains[r, :, 0:128] = peak_w[:128]
        gains[r, :, 128:256] = total_w[:128]
        got = jnp.dot(weights[...], lat[r], preferred_element_type=F32)
        out_a[r] = got[128:].astype(BF16)
        a_copies[r].start()
        mixed[r] = got[:128]

    def combine(r):
        with jax.named_scope(f"waits{r}"):
            s_copies[r].wait_recv()
        peak_0, total_0 = gains[r, :, 0:128], gains[r, :, 128:256]
        peak_1, total_1 = in_s[r, :, 0:128], in_s[r, :, 128:256]
        peak = jnp.maximum(peak_0, peak_1)
        gain_0 = jnp.exp2((peak_0 - peak) * FACTOR)
        gain_1 = jnp.exp2((peak_1 - peak) * FACTOR)
        out_t[r] = stats_tile(peak, total_0 * gain_0 + total_1 * gain_1)
        for copy in t_copies[r]:
            copy.start()
        with jax.named_scope(f"waita{r}"):
            a_copies[r].wait_recv()
        out_b[r] = (mixed[r] * wide(gain_0) + in_a[r].astype(F32) * wide(gain_1)).astype(BF16)
        for copy in b_copies[r]:
            copy.start()

    def finish(r):
        with jax.named_scope(f"waitt{r}"):
            seven(in_t.at[r], t_send.at[r], t_recv.at[r]).wait_recv()
        found = [stats_of(out_t[r, 0:16])] + [
            stats_of(in_t[r, 16 * j : 16 * (j + 1)]) for j in range(1, CHIPS)
        ]
        peak = functools.reduce(jnp.maximum, [p for p, _ in found])
        factors = [jnp.exp2((p - peak) * FACTOR) for p, _ in found]
        total = functools.reduce(jnp.add, [t * f for (_, t), f in zip(found, factors)])
        factors = [jnp.broadcast_to(f / total, (16, LAT)) for f in factors]
        with jax.named_scope(f"waitb{r}"):
            seven(in_b.at[r], b_send.at[r], b_recv.at[r]).wait_recv()
        attended = out_b[r, 0:16].astype(F32) * factors[0]
        for j in range(1, CHIPS):
            attended = attended + in_b[r, 16 * j : 16 * (j + 1)].astype(F32) * factors[j]
        for g in range(4):
            att[g, 16 * r : 16 * (r + 1), :] = attended[:, 128 * g : 128 * (g + 1)]

    with jax.named_scope("scale0"):
        scale(0)
    with jax.named_scope("scale1"):
        scale(1)
    with jax.named_scope("forward0"):
        forward(0)
    with jax.named_scope("scale2"):
        scale(2)
    with jax.named_scope("scale3"):
        scale(3)
    with jax.named_scope("forward1"):
        forward(1)
    with jax.named_scope("waitf0"):
        f_copies[0].wait_recv()
    with jax.named_scope("score0"):
        peak, _ = both(0, None)
    for r in range(R):
        if r + 2 < R:
            with jax.named_scope(f"forward{r+2}"):
                forward(r + 2)
        if r + 1 < R:
            with jax.named_scope(f"waitf{r+1}"):
                f_copies[r + 1].wait_recv()
        with jax.named_scope(f"both{r}"):
            next_peak, total = both(r + 1, peak)
        if r >= 1:
            combine(r - 1)
        with jax.named_scope(f"mix{r}"):
            mix(r, peak, total)
        peak = next_peak
    combine(R - 1)
    for r in range(R):
        finish(r)

    late.wait()
    for h in range(H):
        rows = jnp.concatenate(
            [att[g, pl.ds(h, R * T, stride=H), :] for g in range(4)], axis=1
        ).astype(BF16)
        res[pl.ds(h, R * T, stride=H), :] = jnp.dot(rows, uv_v[h], preferred_element_type=F32)
    out[...] = res[...].reshape(R, T, H, 128).astype(BF16)

    with jax.named_scope("drain"):
        remote(table.at[pl.ds(1, 15)], table.at[pl.ds(1, 15)], table_send, table_recv, partner).wait_send()
        for r in range(R):
            seven(queries.at[r], q_send, q_recv.at[r]).wait_send()
            f_copies[r].wait_send()
            s_copies[r].wait_send()
            a_copies[r].wait_send()
            seven(out_t.at[r], t_send.at[r], t_recv.at[r]).wait_send()
            seven(out_b.at[r], b_send.at[r], b_recv.at[r]).wait_send()


def local(*args):
    dma = pltpu.SemaphoreType.DMA
    return pl.pallas_call(
        kernel,
        out_shape=pltpu.VMEM((R, T, H, 128), BF16),
        in_specs=[pl.BlockSpec(memory_space=pl.ANY)] * 9,
        out_specs=pl.BlockSpec(memory_space=pltpu.VMEM),
        scratch_shapes=[
            pltpu.VMEM((R, T, H, 128), BF16),
            pltpu.VMEM((R, T, H, ROPE), BF16),
            pltpu.VMEM((H, 128, LAT), BF16),
            pltpu.VMEM((H, LAT, 128), BF16),
            pltpu.VMEM((R, SPAN, LAT), BF16),
            pltpu.VMEM((R, ROPE, SPAN), BF16),
            pltpu.VMEM((5, 64), F32),
            pltpu.SMEM((16, 5, 64), F32),
            pltpu.SMEM((R, BLOCKS), jnp.int32),
            pltpu.SMEM((R,), jnp.int32),
            pltpu.VMEM((R * T * H, 128), F32),
            pltpu.VMEM((4, R * T * H, 128), F32),
            pltpu.VMEM((R, ROWS, WIDE), BF16),
            pltpu.VMEM((2, ROWS, SPAN), F32),
            pltpu.VMEM((ROWS, SPAN), BF16),
            pltpu.VMEM((R, 128, LAT), F32),
            pltpu.VMEM((R, 128, 256), F32),
            pltpu.VMEM((R, 128, 256), F32),
            pltpu.VMEM((R, 128, 256), F32),
            pltpu.VMEM((R, 128, LAT), BF16),
            pltpu.VMEM((R, 128, LAT), BF16),
            pltpu.VMEM((R, 128, LAT), BF16),
            pltpu.VMEM((R, 128, LAT), BF16),
            pltpu.VMEM((R, 128, 128), BF16),
            pltpu.VMEM((R, 128, 128), BF16),
            pltpu.VMEM((4, R * T * H, 128), F32),
            pltpu.VMEM((R * T * H, 128), F32),
            dma((8,)),
            dma((R, 2)),
            dma(()),
            dma(()),
            dma(()),
            dma((R,)),
            dma((R,)),
            dma((R,)),
            dma((R,)),
            dma((R,)),
            dma((R,)),
            dma((R,)),
            dma((R,)),
            dma((R,)),
            dma((R,)),
            dma((R,)),
        ],
        compiler_params=pltpu.CompilerParams(collective_id=0, has_side_effects=True),
        name="decode",
    )(*args)


def solution(mesh):
    placed = (
        P("dp", None, "tensor", None),
        P("dp", None, "tensor", None),
        P("tensor", None, None),
        P("tensor", None, None),
        P("dp", "tensor", None),
        P("dp", None, "tensor"),
        P(None, ("dp", "tensor")),
        P("dp", "tensor"),
        P("dp"),
    )
    return jax.shard_map(
        local, mesh=mesh, in_specs=placed, out_specs=P("dp", None, "tensor", None), check_vma=False
    )
```

```python
import functools
import math

import jax
import jax.numpy as jnp
from jax import lax
from jax.experimental import pallas as pl
from jax.experimental.pallas import tpu as pltpu
from jax.sharding import PartitionSpec as P

MESH = pl.DeviceIdType.MESH
R, T, H = 4, 2, 8
ROWS, LAT, ROPE = 256, 512, 64
SPAN, BLOCKS = 2048, 16
X, CHIPS = 4, 8
FACTOR = (128 + 64) ** -0.5 * math.log2(math.e)
MASKED = -1e30
UNROLL = 4
SCALE_UNROLL = 4
F32, BF16 = jnp.float32, jnp.bfloat16


ORDER = (6, 2, 5, 7, 1, 3, 4, 0)
WIDTH = 512
CHUNKS = SPAN // WIDTH


def stats_rows(peak, total):
    lane = lax.broadcasted_iota(jnp.int32, (CHIPS, 16, 128), 2)
    at = lax.broadcasted_iota(jnp.int32, (CHIPS, 16, 128), 1)
    spread = jnp.where(
        lane == at, peak.reshape(CHIPS, 16, 128), jnp.where(lane == at + 16, total.reshape(CHIPS, 16, 128), 0.0)
    )
    return jnp.sum(spread, axis=1)


def wide(tile):
    return jnp.concatenate([tile] * 4, axis=1)


def kernel(
    q_nope, q_rope, w_uk, w_uv, latent, rope, pool, index, lengths, out,
    nope_v, qrope_v, uk_v, uv_v, lat, rop, pool_v, table, index_s, length_s,
    qf, flat, queries, turns, scores, weights, mixed, out_s, in_s, gains,
    out_a, in_a, out_b, in_b, out_t, in_t, att, res,
    load_sem, lat_sem, table_send, table_recv, q_send, q_recv, o_send, o_recv, f_send, f_recv, g_send, g_recv,
    s_send, s_recv, a_send, a_recv, t_send, t_recv, b_send, b_recv,
):
    me = lax.axis_index("tensor")
    core = lax.rem(me, 2)
    chip = me // 2
    row, column = chip // X, lax.rem(chip, X)
    partner = me + 1 - 2 * core

    def peer(j, sign):
        dy, dx = j // X, j % X
        other = lax.rem(row + dy, 2) * X + lax.rem(column + (dx if sign > 0 else X - dx), X)
        return other * 2 + 1 - core

    def remote(src, dst, send, recv, to):
        return pltpu.make_async_remote_copy(
            src_ref=src, dst_ref=dst, send_sem=send, recv_sem=recv,
            device_id={"tensor": to}, device_id_type=MESH,
        )

    def eight(ref, send, recv):
        return remote(ref.at[pl.ds(0, 128)], ref.at[pl.ds(0, 128)], send, recv, partner)

    barrier = pltpu.get_barrier_semaphore()
    for step in range(1, 16):
        pl.semaphore_signal(
            barrier, inc=1, device_id={"tensor": lax.rem(me + step, 16)}, device_id_type=MESH
        )

    small = [
        pltpu.make_async_copy(w_uk, uk_v, load_sem.at[0]),
        pltpu.make_async_copy(q_nope, nope_v, load_sem.at[1]),
        pltpu.make_async_copy(q_rope, qrope_v, load_sem.at[2]),
        pltpu.make_async_copy(pool, pool_v, load_sem.at[3]),
        pltpu.make_async_copy(index, index_s, load_sem.at[4]),
        pltpu.make_async_copy(lengths, length_s, load_sem.at[5]),
    ]
    big = [pltpu.make_async_copy(latent.at[r], lat.at[r], lat_sem.at[r]) for r in range(R)]
    big.insert(1, pltpu.make_async_copy(rope, rop, lat_sem.at[R]))
    late = pltpu.make_async_copy(w_uv, uv_v, load_sem.at[6])
    for copy in small:
        copy.start()
    with jax.named_scope("waitsmall"):
        for copy in small:
            copy.wait()
    own_table = pltpu.make_async_copy(pool_v, table.at[0], load_sem.at[7])
    for copy in [own_table] + big + [late]:
        copy.start()
    qf[...] = nope_v[...].astype(F32).reshape(R * T * H, 128)
    for h in range(H):
        rows = qf[pl.ds(h, R * T, stride=H), :].astype(BF16)
        got = jnp.dot(rows, uk_v[h], preferred_element_type=F32)
        for g in range(4):
            flat[g, pl.ds(h, R * T, stride=H), :] = got[:, 128 * g : 128 * (g + 1)]
    for r in range(R):
        for g in range(4):
            queries[r, 128:144, 128 * g : 128 * (g + 1)] = flat[g, 16 * r : 16 * (r + 1), :].astype(BF16)

    for pair in range(R // 2):
        turned = [qrope_v[2 * pair + n].astype(F32).reshape(16, ROPE) for n in range(2)]
        turns[pair, 128:144] = jnp.concatenate(turned, axis=1).astype(BF16)

    with jax.named_scope("barrier"):
        pl.semaphore_wait(barrier, 15)
    table_copies = [
        remote(pool_v, table.at[step], table_send, table_recv, lax.rem(me + 16 - step, 16))
        for step in (8, 7, 9, 4, 5, 12, 11, 13, 3, 6, 10, 2, 14, 1, 15)
    ]
    for copy in table_copies:
        copy.start()

    q_copies = [
        [
            remote(queries.at[r, pl.ds(128, 16)], queries.at[r, pl.ds(16 * j, 16)],
                   q_send, q_recv.at[r], peer(j, -1))
            for j in ORDER
        ]
        for r in range(R)
    ]
    o_copies = [
        [
            remote(turns.at[p, pl.ds(128, 16)], turns.at[p, pl.ds(16 * j, 16)], o_send, o_recv.at[p], peer(j, -1))
            for j in ORDER
        ]
        for p in range(R // 2)
    ]
    for r in range(R):
        for at in range(CHIPS):
            if r % 2 == 0:
                o_copies[r // 2][at].start()
            q_copies[r][at].start()
    g_copies = [
        remote(turns.at[p, pl.ds(16, 112)], turns.at[p, pl.ds(144, 112)], g_send, g_recv.at[p], partner)
        for p in range(R // 2)
    ]
    f_copies = [
        remote(queries.at[r, pl.ds(16, 112)], queries.at[r, pl.ds(144, 112)],
               f_send, f_recv.at[r], partner)
        for r in range(R)
    ]
    s_copies = [
        remote(out_s.at[r], in_s.at[r], s_send, s_recv.at[r], partner) for r in range(R)
    ]
    a_copies = [
        remote(out_a.at[r], in_a.at[r], a_send, a_recv.at[r], partner) for r in range(R)
    ]
    t_copies = [
        [
            remote(out_t.at[r, pl.ds(j, 1)], in_t.at[r, pl.ds(j, 1)],
                   t_send, t_recv.at[r], peer(j, 1))
            for j in ORDER
        ]
        for r in range(R)
    ]
    b_copies = [
        [
            remote(out_b.at[r, pl.ds(16 * j, 16)], in_b.at[r, pl.ds(16 * j, 16)],
                   b_send, b_recv.at[r], peer(j, 1))
            for j in ORDER
        ]
        for r in range(R)
    ]

    def forward(r):
        if r % 2 == 0:
            eight(turns.at[r // 2], o_send, o_recv.at[r // 2]).wait_recv()
            g_copies[r // 2].start()
        eight(queries.at[r], q_send, q_recv.at[r]).wait_recv()
        f_copies[r].start()

    def forwarded(r):
        if r % 2 == 0:
            g_copies[r // 2].wait_recv()
        f_copies[r].wait_recv()

    with jax.named_scope("waittable"):
        remote(table.at[pl.ds(1, 15)], table.at[pl.ds(1, 15)], table_send, table_recv, partner).wait_recv()
        own_table.wait()

    def scale_block(r, b):
        at = index_s[r, b]
        slot = lax.rem(at // 64 + 16 - me, 16)
        col = lax.rem(at, 64)
        rows = pl.ds(pl.multiple_of(b * 128, 128), 128)
        for g in range(4):
            lat[r, rows, 128 * g : 128 * (g + 1)] = (
                lat[r, rows, 128 * g : 128 * (g + 1)].astype(F32) * table[slot, g, col]
            ).astype(BF16)
        rop[r, :, rows] = (rop[r, :, rows].astype(F32) * table[slot, 4, col]).astype(BF16)

    def scale(r, first=0, last=BLOCKS):
        if first == 0:
            big[r + 1 if r else 0].wait()
            if r == 0:
                big[1].wait()

        def one(b, carry):
            scale_block(r, b)
            return carry

        lax.fori_loop(first, last, one, 0, unroll=SCALE_UNROLL)

    def score(r, n, top):
        cols = pl.ds(pl.multiple_of(n * WIDTH, WIDTH), WIDTH)
        got = lax.dot_general(
            queries[r], lat[r, cols, :], (((1,), (1,)), ((), ())),
            preferred_element_type=F32,
        ) + jnp.dot(
            turns[r // 2, :, ROPE * (r % 2) : ROPE * (r % 2 + 1)], rop[r, :, cols], preferred_element_type=F32
        )
        place = lax.broadcasted_iota(jnp.int32, (1, T, 8, WIDTH), 3) + (me * SPAN + n * WIDTH)
        limit = length_s[r] - T + lax.broadcasted_iota(jnp.int32, (1, T, 8, WIDTH), 1)
        got = jnp.where(place <= limit, got.reshape(16, T, 8, WIDTH), MASKED).reshape(ROWS, WIDTH)
        scores[r % 2, :, cols] = got
        for g in range(WIDTH // 128):
            top = jnp.maximum(top, got[:, 128 * g : 128 * (g + 1)])
        return top

    def weigh(r, n, peak, total):
        cols = pl.ds(pl.multiple_of(n * WIDTH, WIDTH), WIDTH)
        got = jnp.exp2((scores[r % 2, :, cols] - peak) * FACTOR)
        weights[:, cols] = got.astype(BF16)
        for g in range(WIDTH // 128):
            total = total + got[:, 128 * g : 128 * (g + 1)]
        return total

    def both(r, peak, beside=None):
        top, total = jnp.full((ROWS, 128), -3e38, F32), jnp.zeros((ROWS, 128), F32)

        def one(n, carry):
            top, total = carry
            if r < R:
                top = score(r, n, top)
            if r > 0:
                total = weigh(r - 1, n, peak, total)
            if beside is not None:
                for b in range(BLOCKS // CHUNKS):
                    scale_block(beside, n * (BLOCKS // CHUNKS) + b)
            return top, total

        top, total = lax.fori_loop(0, CHUNKS, one, (top, total), unroll=UNROLL)
        if r < R:
            top = jnp.max(top, axis=1, keepdims=True)
        if r > 0:
            total = jnp.sum(total, axis=1, keepdims=True)
        return top, total

    def mix(r, peak, total):
        peak_w = jnp.broadcast_to(peak, (ROWS, 128))
        total_w = jnp.broadcast_to(total, (ROWS, 128))
        out_s[r, :, 0:128] = peak_w[128:]
        out_s[r, :, 128:256] = total_w[128:]
        s_copies[r].start()
        gains[r, :, 0:128] = peak_w[:128]
        gains[r, :, 128:256] = total_w[:128]
        got = jnp.dot(weights[...], lat[r], preferred_element_type=F32)
        out_a[r] = got[128:].astype(BF16)
        a_copies[r].start()
        mixed[r] = got[:128]

    def combine(r):
        with jax.named_scope(f"waits{r}"):
            s_copies[r].wait_recv()
        peak_0, total_0 = gains[r, :, 0:128], gains[r, :, 128:256]
        peak_1, total_1 = in_s[r, :, 0:128], in_s[r, :, 128:256]
        peak = jnp.maximum(peak_0, peak_1)
        gain_0 = jnp.exp2((peak_0 - peak) * FACTOR)
        gain_1 = jnp.exp2((peak_1 - peak) * FACTOR)
        out_t[r] = stats_rows(peak, total_0 * gain_0 + total_1 * gain_1)
        for copy in t_copies[r]:
            copy.start()
        with jax.named_scope(f"waita{r}"):
            a_copies[r].wait_recv()
        out_b[r] = (mixed[r] * wide(gain_0) + in_a[r].astype(F32) * wide(gain_1)).astype(BF16)
        for copy in b_copies[r]:
            copy.start()

    def finish(r):
        with jax.named_scope(f"waitt{r}"):
            remote(out_t.at[r], in_t.at[r], t_send, t_recv.at[r], partner).wait_recv()
        found = in_t[r]
        factors = jnp.exp2((found - jnp.max(found, axis=0, keepdims=True)) * FACTOR)
        total = jnp.sum(factors * pltpu.roll(found, 112, 1), axis=0, keepdims=True)
        lane = lax.broadcasted_iota(jnp.int32, (CHIPS, 128), 1)
        factors = jnp.transpose(jnp.where(lane < 16, factors / total, 0.0))[0:16]
        factors = [jnp.broadcast_to(factors[:, j : j + 1], (16, LAT)) for j in range(CHIPS)]
        with jax.named_scope(f"waitb{r}"):
            eight(in_b.at[r], b_send, b_recv.at[r]).wait_recv()
        attended = jnp.zeros((16, LAT), F32)
        for j in range(CHIPS):
            attended = attended + in_b[r, 16 * j : 16 * (j + 1)].astype(F32) * factors[j]
        for g in range(4):
            att[g, 16 * r : 16 * (r + 1), :] = attended[:, 128 * g : 128 * (g + 1)]

    with jax.named_scope("scale0"):
        scale(0)
    with jax.named_scope("scale1"):
        scale(1, 0, 8)
    with jax.named_scope("forward0"):
        forward(0)
    with jax.named_scope("scale2"):
        scale(1, 8, 16)
        scale(2)
    with jax.named_scope("scale3"):
        scale(3)
    with jax.named_scope("forward1"):
        forward(1)
    with jax.named_scope("waitf0"):
        forwarded(0)
    with jax.named_scope("score0"):
        peak, _ = both(0, None)
    for r in range(R):
        if r + 2 < R:
            with jax.named_scope(f"forward{r+2}"):
                forward(r + 2)
        if r + 1 < R:
            with jax.named_scope(f"waitf{r+1}"):
                forwarded(r + 1)
        with jax.named_scope(f"both{r}"):
            next_peak, total = both(r + 1, peak)
        if 1 <= r < R - 1:
            combine(r - 1)
        with jax.named_scope(f"mix{r}"):
            mix(r, peak, total)
        if r == R - 1:
            combine(r - 1)
        peak = next_peak
    combine(R - 1)
    for r in range(R):
        finish(r)

    late.wait()
    for h in range(H):
        rows = jnp.concatenate(
            [att[g, pl.ds(h, R * T, stride=H), :] for g in range(4)], axis=1
        ).astype(BF16)
        res[pl.ds(h, R * T, stride=H), :] = jnp.dot(rows, uv_v[h], preferred_element_type=F32)
    out[...] = res[...].reshape(R, T, H, 128).astype(BF16)

    with jax.named_scope("drain"):
        remote(table.at[pl.ds(1, 15)], table.at[pl.ds(1, 15)], table_send, table_recv, partner).wait_send()
        for ref, rows, send in (
            (queries, pl.ds(0, 128), q_send), (turns, pl.ds(0, 128), o_send), (turns, pl.ds(16, 112), g_send),
            (queries, pl.ds(16, 112), f_send), (out_s, pl.ds(0, 128), s_send),
            (out_a, pl.ds(0, 128), a_send), (out_t, pl.ds(0, 8), t_send), (out_b, pl.ds(0, 128), b_send),
        ):
            remote(ref.at[:, rows], ref.at[:, rows], send, table_recv, partner).wait_send()


def local(*args):
    dma = pltpu.SemaphoreType.DMA
    return pl.pallas_call(
        kernel,
        out_shape=pltpu.VMEM((R, T, H, 128), BF16),
        in_specs=[pl.BlockSpec(memory_space=pl.ANY)] * 9,
        out_specs=pl.BlockSpec(memory_space=pltpu.VMEM),
        scratch_shapes=[
            pltpu.VMEM((R, T, H, 128), BF16),
            pltpu.VMEM((R, T, H, ROPE), BF16),
            pltpu.VMEM((H, 128, LAT), BF16),
            pltpu.VMEM((H, LAT, 128), BF16),
            pltpu.VMEM((R, SPAN, LAT), BF16),
            pltpu.VMEM((R, ROPE, SPAN), BF16),
            pltpu.VMEM((5, 64), F32),
            pltpu.SMEM((16, 5, 64), F32),
            pltpu.SMEM((R, BLOCKS), jnp.int32),
            pltpu.SMEM((R,), jnp.int32),
            pltpu.VMEM((R * T * H, 128), F32),
            pltpu.VMEM((4, R * T * H, 128), F32),
            pltpu.VMEM((R, ROWS, LAT), BF16),
            pltpu.VMEM((R // 2, ROWS, 128), BF16),
            pltpu.VMEM((2, ROWS, SPAN), F32),
            pltpu.VMEM((ROWS, SPAN), BF16),
            pltpu.VMEM((R, 128, LAT), F32),
            pltpu.VMEM((R, 128, 256), F32),
            pltpu.VMEM((R, 128, 256), F32),
            pltpu.VMEM((R, 128, 256), F32),
            pltpu.VMEM((R, 128, LAT), BF16),
            pltpu.VMEM((R, 128, LAT), BF16),
            pltpu.VMEM((R, 128, LAT), BF16),
            pltpu.VMEM((R, 128, LAT), BF16),
            pltpu.VMEM((R, CHIPS, 128), F32),
            pltpu.VMEM((R, CHIPS, 128), F32),
            pltpu.VMEM((4, R * T * H, 128), F32),
            pltpu.VMEM((R * T * H, 128), F32),
            dma((8,)),
            dma((R + 1,)),
            dma(()),
            dma(()),
            dma(()),
            dma((R,)),
            dma(()),
            dma((R // 2,)),
            dma(()),
            dma((R,)),
            dma(()),
            dma((R // 2,)),
            dma(()),
            dma((R,)),
            dma(()),
            dma((R,)),
            dma(()),
            dma((R,)),
            dma(()),
            dma((R,)),
        ],
        compiler_params=pltpu.CompilerParams(collective_id=0, has_side_effects=True),
        name="decode",
    )(*args)


def solution(mesh):
    placed = (
        P("dp", None, "tensor", None),
        P("dp", None, "tensor", None),
        P("tensor", None, None),
        P("tensor", None, None),
        P("dp", "tensor", None),
        P("dp", None, "tensor"),
        P(None, ("dp", "tensor")),
        P("dp", "tensor"),
        P("dp"),
    )
    return jax.shard_map(
        local, mesh=mesh, in_specs=placed, out_specs=P("dp", None, "tensor", None), check_vma=False
    )
```

```python
import functools
import math

import jax
import jax.numpy as jnp
from jax import lax
from jax.experimental import pallas as pl
from jax.experimental.pallas import tpu as pltpu
from jax.sharding import PartitionSpec as P

MESH = pl.DeviceIdType.MESH
R, T, H = 4, 2, 8
ROWS, LAT, ROPE = 256, 512, 64
SPAN, BLOCKS = 2048, 16
X, CHIPS = 4, 8
FACTOR = (128 + 64) ** -0.5 * math.log2(math.e)
MASKED = -1e30
MERGE = True
SPLIT = 8
SCALE_UNROLL = 4
F32, BF16 = jnp.float32, jnp.bfloat16


ORDER = (6, 2, 5, 7, 1, 3, 4, 0)
WIDTH = 512
CHUNKS = SPAN // WIDTH


def stats_rows(peak, total):
    lane = lax.broadcasted_iota(jnp.int32, (CHIPS, 16, 128), 2)
    at = lax.broadcasted_iota(jnp.int32, (CHIPS, 16, 128), 1)
    spread = jnp.where(
        lane == at, peak.reshape(CHIPS, 16, 128), jnp.where(lane == at + 16, total.reshape(CHIPS, 16, 128), 0.0)
    )
    return jnp.sum(spread, axis=1)


def wide(tile):
    return jnp.concatenate([tile] * 4, axis=1)


def kernel(
    q_nope, q_rope, w_uk, w_uv, latent, rope, pool, index, lengths, out,
    nope_v, qrope_v, uk_v, uv_v, lat, rop, pool_v, table, index_s, length_s,
    qf, flat, queries, turns, scores, weights, mixed, out_s, in_s, gains,
    out_a, in_a, out_b, in_b, out_t, in_t, att, res,
    load_sem, lat_sem, table_send, table_recv, q_send, q_recv, o_send, o_recv, f_send, f_recv, g_send, g_recv,
    s_send, s_recv, a_send, a_recv, t_send, t_recv, b_send, b_recv,
):
    me = lax.axis_index("tensor")
    core = lax.rem(me, 2)
    chip = me // 2
    row, column = chip // X, lax.rem(chip, X)
    partner = me + 1 - 2 * core

    def peer(j, sign):
        dy, dx = j // X, j % X
        other = lax.rem(row + dy, 2) * X + lax.rem(column + (dx if sign > 0 else X - dx), X)
        return other * 2 + 1 - core

    def remote(src, dst, send, recv, to):
        return pltpu.make_async_remote_copy(
            src_ref=src, dst_ref=dst, send_sem=send, recv_sem=recv,
            device_id={"tensor": to}, device_id_type=MESH,
        )

    def eight(ref, send, recv):
        return remote(ref.at[pl.ds(0, 128)], ref.at[pl.ds(0, 128)], send, recv, partner)

    barrier = pltpu.get_barrier_semaphore()
    for step in range(1, 16):
        pl.semaphore_signal(
            barrier, inc=1, device_id={"tensor": lax.rem(me + step, 16)}, device_id_type=MESH
        )

    small = [
        pltpu.make_async_copy(w_uk, uk_v, load_sem.at[0]),
        pltpu.make_async_copy(q_nope, nope_v, load_sem.at[1]),
        pltpu.make_async_copy(q_rope, qrope_v, load_sem.at[2]),
        pltpu.make_async_copy(pool, pool_v, load_sem.at[3]),
        pltpu.make_async_copy(index, index_s, load_sem.at[4]),
        pltpu.make_async_copy(lengths, length_s, load_sem.at[5]),
    ]
    big = [pltpu.make_async_copy(latent.at[r], lat.at[r], lat_sem.at[r]) for r in range(R)]
    big.insert(1, pltpu.make_async_copy(rope, rop, lat_sem.at[R]))
    late = pltpu.make_async_copy(w_uv, uv_v, load_sem.at[6])
    for copy in small:
        copy.start()
    with jax.named_scope("waitsmall"):
        for copy in small:
            copy.wait()
    own_table = pltpu.make_async_copy(pool_v, table.at[0], load_sem.at[7])
    for copy in [own_table] + big + [late]:
        copy.start()
    qf[...] = nope_v[...].astype(F32).reshape(R * T * H, 128)
    for h in range(H):
        rows = qf[pl.ds(h, R * T, stride=H), :].astype(BF16)
        got = jnp.dot(rows, uk_v[h], preferred_element_type=F32)
        for g in range(4):
            flat[g, pl.ds(h, R * T, stride=H), :] = got[:, 128 * g : 128 * (g + 1)]
    for r in range(R):
        for g in range(4):
            queries[r, 128:144, 128 * g : 128 * (g + 1)] = flat[g, 16 * r : 16 * (r + 1), :].astype(BF16)

    for pair in range(R // 2):
        turned = [qrope_v[2 * pair + n].astype(F32).reshape(16, ROPE) for n in range(2)]
        turns[pair, 128:144] = jnp.concatenate(turned, axis=1).astype(BF16)

    with jax.named_scope("barrier"):
        pl.semaphore_wait(barrier, 15)
    table_copies = [
        remote(pool_v, table.at[step], table_send, table_recv, lax.rem(me + 16 - step, 16))
        for step in (8, 7, 9, 4, 5, 12, 11, 13, 3, 6, 10, 2, 14, 1, 15)
    ]
    for copy in table_copies:
        copy.start()

    q_copies = [
        [
            remote(queries.at[r, pl.ds(128, 16)], queries.at[r, pl.ds(16 * j, 16)],
                   q_send, q_recv.at[r], peer(j, -1))
            for j in ORDER
        ]
        for r in range(R)
    ]
    o_copies = [
        [
            remote(turns.at[p, pl.ds(128, 16)], turns.at[p, pl.ds(16 * j, 16)], o_send, o_recv.at[p], peer(j, -1))
            for j in ORDER
        ]
        for p in range(R // 2)
    ]
    def ask(r):
        for at in range(CHIPS):
            if r % 2 == 0:
                o_copies[r // 2][at].start()
            q_copies[r][at].start()

    ask(0)
    ask(1)
    ask(2)
    ask(3)
    g_copies = [
        remote(turns.at[p, pl.ds(16, 112)], turns.at[p, pl.ds(144, 112)], g_send, g_recv.at[p], partner)
        for p in range(R // 2)
    ]
    f_copies = [
        remote(queries.at[r, pl.ds(16, 112)], queries.at[r, pl.ds(144, 112)],
               f_send, f_recv.at[r], partner)
        for r in range(R)
    ]
    s_copies = [
        remote(out_s.at[r], in_s.at[r], s_send, s_recv.at[r], partner) for r in range(R)
    ]
    a_copies = [
        remote(out_a.at[r], in_a.at[r], a_send, a_recv.at[r], partner) for r in range(R)
    ]
    t_copies = [
        [
            remote(out_t.at[r, pl.ds(j, 1)], in_t.at[r, pl.ds(j, 1)],
                   t_send, t_recv.at[r], peer(j, 1))
            for j in ORDER
        ]
        for r in range(R)
    ]
    b_copies = [
        [
            remote(out_b.at[r, pl.ds(16 * j, 16)], in_b.at[r, pl.ds(16 * j, 16)],
                   b_send, b_recv.at[r], peer(j, 1))
            for j in ORDER
        ]
        for r in range(R)
    ]

    def forward(r):
        if r % 2 == 0:
            eight(turns.at[r // 2], o_send, o_recv.at[r // 2]).wait_recv()
            g_copies[r // 2].start()
        eight(queries.at[r], q_send, q_recv.at[r]).wait_recv()
        f_copies[r].start()

    def forwarded(r):
        if r % 2 == 0:
            g_copies[r // 2].wait_recv()
        f_copies[r].wait_recv()

    with jax.named_scope("waittable"):
        remote(table.at[pl.ds(1, 15)], table.at[pl.ds(1, 15)], table_send, table_recv, partner).wait_recv()
        own_table.wait()

    def scale_block(r, b):
        at = index_s[r, b]
        slot = lax.rem(at // 64 + 16 - me, 16)
        col = lax.rem(at, 64)
        rows = pl.ds(pl.multiple_of(b * 128, 128), 128)
        for g in range(4):
            lat[r, rows, 128 * g : 128 * (g + 1)] = (
                lat[r, rows, 128 * g : 128 * (g + 1)].astype(F32) * table[slot, g, col]
            ).astype(BF16)
        rop[r, :, rows] = (rop[r, :, rows].astype(F32) * table[slot, 4, col]).astype(BF16)

    def scale(r, first=0, last=BLOCKS):
        if first == 0 and last > 0:
            big[r + 1 if r else 0].wait()
            if r == 0:
                big[1].wait()

        def one(b, carry):
            scale_block(r, b)
            return carry

        lax.fori_loop(first, last, one, 0, unroll=SCALE_UNROLL)

    def score(r, n, top):
        cols = pl.ds(n * WIDTH, WIDTH)
        got = lax.dot_general(
            queries[r], lat[r, cols, :], (((1,), (1,)), ((), ())),
            preferred_element_type=F32,
        ) + jnp.dot(
            turns[r // 2, :, ROPE * (r % 2) : ROPE * (r % 2 + 1)], rop[r, :, cols], preferred_element_type=F32
        )
        place = lax.broadcasted_iota(jnp.int32, (1, T, 8, WIDTH), 3) + (me * SPAN + n * WIDTH)
        limit = length_s[r] - T + lax.broadcasted_iota(jnp.int32, (1, T, 8, WIDTH), 1)
        got = jnp.where(place <= limit, got.reshape(16, T, 8, WIDTH), MASKED).reshape(ROWS, WIDTH)
        scores[r % 2, :, cols] = got
        for g in range(WIDTH // 128):
            top = jnp.maximum(top, got[:, 128 * g : 128 * (g + 1)])
        return top

    def weigh(r, n, peak, total):
        cols = pl.ds(n * WIDTH, WIDTH)
        got = jnp.exp2((scores[r % 2, :, cols] - peak) * FACTOR)
        weights[:, cols] = got.astype(BF16)
        for g in range(WIDTH // 128):
            total = total + got[:, 128 * g : 128 * (g + 1)]
        return total

    def look(r, between=None):
        top = jnp.full((ROWS, 128), -3e38, F32)
        for n in range(CHUNKS):
            if between is not None and n == between[0]:
                between[1]()
            top = score(r, n, top)
        return jnp.max(top, axis=1, keepdims=True)

    def tell(r, peak, total):
        peak_w = jnp.broadcast_to(peak, (ROWS, 128))
        total_w = jnp.broadcast_to(total, (ROWS, 128))
        out_s[r, :, 0:128] = peak_w[128:]
        out_s[r, :, 128:256] = total_w[128:]
        s_copies[r].start()
        gains[r, :, 0:128] = peak_w[:128]
        gains[r, :, 128:256] = total_w[:128]

    def keep(r, got):
        out_a[r] = got[128:].astype(BF16)
        a_copies[r].start()
        mixed[r] = got[:128]

    def factors_of(r):
        peak_0, total_0 = gains[r, :, 0:128], gains[r, :, 128:256]
        peak_1, total_1 = in_s[r, :, 0:128], in_s[r, :, 128:256]
        peak = jnp.maximum(peak_0, peak_1)
        gain_0 = jnp.exp2((peak_0 - peak) * FACTOR)
        gain_1 = jnp.exp2((peak_1 - peak) * FACTOR)
        out_t[r] = stats_rows(peak, total_0 * gain_0 + total_1 * gain_1)
        return gain_0, gain_1

    def join(r, gain_0, gain_1):
        out_b[r] = (mixed[r] * wide(gain_0) + in_a[r].astype(F32) * wide(gain_1)).astype(BF16)

    def combine(r):
        with jax.named_scope(f"waits{r}"):
            s_copies[r].wait_recv()
        both_gains = factors_of(r)
        for copy in t_copies[r]:
            copy.start()
        with jax.named_scope(f"waita{r}"):
            a_copies[r].wait_recv()
        join(r, *both_gains)
        for copy in b_copies[r]:
            copy.start()

    def mix(r, peak):
        if r >= 1 and MERGE:
            with jax.named_scope(f"waitsa{r-1}"):
                s_copies[r - 1].wait_recv()
                a_copies[r - 1].wait_recv()
        elif r >= 1:
            combine(r - 1)
        with jax.named_scope(f"mix{r}"):
            total, got = jnp.zeros((ROWS, 128), F32), None
            for n in range(CHUNKS):
                total = weigh(r, n, peak, total)
            if r >= 1 and MERGE:
                join(r - 1, *factors_of(r - 1))
            for n in range(CHUNKS):
                cols = pl.ds(n * WIDTH, WIDTH)
                one = jnp.dot(weights[:, cols], lat[r, cols, :], preferred_element_type=F32)
                got = one if got is None else got + one
            if r >= 1 and MERGE:
                for copy in t_copies[r - 1] + b_copies[r - 1]:
                    copy.start()
            tell(r, peak, jnp.sum(total, axis=1, keepdims=True))
            keep(r, got)

    def finish(r):
        with jax.named_scope(f"waitt{r}"):
            remote(out_t.at[r], in_t.at[r], t_send, t_recv.at[r], partner).wait_recv()
        found = in_t[r]
        factors = jnp.exp2((found - jnp.max(found, axis=0, keepdims=True)) * FACTOR)
        total = jnp.sum(factors * pltpu.roll(found, 112, 1), axis=0, keepdims=True)
        lane = lax.broadcasted_iota(jnp.int32, (CHIPS, 128), 1)
        factors = jnp.transpose(jnp.where(lane < 16, factors / total, 0.0))[0:16]
        factors = [jnp.broadcast_to(factors[:, j : j + 1], (16, LAT)) for j in range(CHIPS)]
        with jax.named_scope(f"waitb{r}"):
            eight(in_b.at[r], b_send, b_recv.at[r]).wait_recv()
        attended = jnp.zeros((16, LAT), F32)
        for j in range(CHIPS):
            attended = attended + in_b[r, 16 * j : 16 * (j + 1)].astype(F32) * factors[j]
        for g in range(4):
            att[g, 16 * r : 16 * (r + 1), :] = attended[:, 128 * g : 128 * (g + 1)]

    with jax.named_scope("scale0"):
        scale(0)
    with jax.named_scope("scale1"):
        scale(1, 0, 8)
    with jax.named_scope("forward0"):
        forward(0)
    with jax.named_scope("scale2"):
        scale(1, 8, 16)
        scale(2)
    scale(3, 0, SPLIT)
    for r in range(R):
        with jax.named_scope(f"waitf{r}"):
            forwarded(r)
        with jax.named_scope(f"score{r}"):
            peak = look(r, (1, functools.partial(forward, r + 1)) if r + 1 < R else None)
        if r == 0:
            with jax.named_scope("scale3"):
                scale(3, SPLIT, BLOCKS)
        mix(r, peak)
    combine(R - 1)
    for r in range(R):
        finish(r)

    late.wait()
    for h in range(H):
        rows = jnp.concatenate(
            [att[g, pl.ds(h, R * T, stride=H), :] for g in range(4)], axis=1
        ).astype(BF16)
        res[pl.ds(h, R * T, stride=H), :] = jnp.dot(rows, uv_v[h], preferred_element_type=F32)
    out[...] = res[...].reshape(R, T, H, 128).astype(BF16)

    with jax.named_scope("drain"):
        remote(table.at[pl.ds(1, 15)], table.at[pl.ds(1, 15)], table_send, table_recv, partner).wait_send()
        for ref, rows, send in (
            (queries, pl.ds(0, 128), q_send), (turns, pl.ds(0, 128), o_send), (turns, pl.ds(16, 112), g_send),
            (queries, pl.ds(16, 112), f_send), (out_s, pl.ds(0, 128), s_send),
            (out_a, pl.ds(0, 128), a_send), (out_t, pl.ds(0, 8), t_send), (out_b, pl.ds(0, 128), b_send),
        ):
            remote(ref.at[:, rows], ref.at[:, rows], send, table_recv, partner).wait_send()


def local(*args):
    dma = pltpu.SemaphoreType.DMA
    return pl.pallas_call(
        kernel,
        out_shape=pltpu.VMEM((R, T, H, 128), BF16),
        in_specs=[pl.BlockSpec(memory_space=pl.ANY)] * 9,
        out_specs=pl.BlockSpec(memory_space=pltpu.VMEM),
        scratch_shapes=[
            pltpu.VMEM((R, T, H, 128), BF16),
            pltpu.VMEM((R, T, H, ROPE), BF16),
            pltpu.VMEM((H, 128, LAT), BF16),
            pltpu.VMEM((H, LAT, 128), BF16),
            pltpu.VMEM((R, SPAN, LAT), BF16),
            pltpu.VMEM((R, ROPE, SPAN), BF16),
            pltpu.VMEM((5, 64), F32),
            pltpu.SMEM((16, 5, 64), F32),
            pltpu.SMEM((R, BLOCKS), jnp.int32),
            pltpu.SMEM((R,), jnp.int32),
            pltpu.VMEM((R * T * H, 128), F32),
            pltpu.VMEM((4, R * T * H, 128), F32),
            pltpu.VMEM((R, ROWS, LAT), BF16),
            pltpu.VMEM((R // 2, ROWS, 128), BF16),
            pltpu.VMEM((2, ROWS, SPAN), F32),
            pltpu.VMEM((ROWS, SPAN), BF16),
            pltpu.VMEM((R, 128, LAT), F32),
            pltpu.VMEM((R, 128, 256), F32),
            pltpu.VMEM((R, 128, 256), F32),
            pltpu.VMEM((R, 128, 256), F32),
            pltpu.VMEM((R, 128, LAT), BF16),
            pltpu.VMEM((R, 128, LAT), BF16),
            pltpu.VMEM((R, 128, LAT), BF16),
            pltpu.VMEM((R, 128, LAT), BF16),
            pltpu.VMEM((R, CHIPS, 128), F32),
            pltpu.VMEM((R, CHIPS, 128), F32),
            pltpu.VMEM((4, R * T * H, 128), F32),
            pltpu.VMEM((R * T * H, 128), F32),
            dma((8,)),
            dma((R + 1,)),
            dma(()),
            dma(()),
            dma(()),
            dma((R,)),
            dma(()),
            dma((R // 2,)),
            dma(()),
            dma((R,)),
            dma(()),
            dma((R // 2,)),
            dma(()),
            dma((R,)),
            dma(()),
            dma((R,)),
            dma(()),
            dma((R,)),
            dma(()),
            dma((R,)),
        ],
        compiler_params=pltpu.CompilerParams(collective_id=0, has_side_effects=True),
        name="decode",
    )(*args)


def solution(mesh):
    placed = (
        P("dp", None, "tensor", None),
        P("dp", None, "tensor", None),
        P("tensor", None, None),
        P("tensor", None, None),
        P("dp", "tensor", None),
        P("dp", None, "tensor"),
        P(None, ("dp", "tensor")),
        P("dp", "tensor"),
        P("dp"),
    )
    return jax.shard_map(
        local, mesh=mesh, in_specs=placed, out_specs=P("dp", None, "tensor", None), check_vma=False
    )
```

```python
import functools
import math

import jax
import jax.numpy as jnp
from jax import lax
from jax.experimental import pallas as pl
from jax.experimental.pallas import tpu as pltpu
from jax.sharding import PartitionSpec as P

MESH = pl.DeviceIdType.MESH
R, T, H = 4, 2, 8
ROWS, LAT, ROPE = 256, 512, 64
SPAN, BLOCKS = 2048, 16
X, CHIPS = 4, 8
FACTOR = (128 + 64) ** -0.5 * math.log2(math.e)
MASKED = -1e30
MERGE = True
SPLIT = 8
SCALE_UNROLL = 4
F32, BF16 = jnp.float32, jnp.bfloat16


ORDER = (6, 2, 5, 7, 1, 3, 4, 0)
WIDTH = 512
CHUNKS = SPAN // WIDTH


def stats_rows(peak, total):
    lane = lax.broadcasted_iota(jnp.int32, (CHIPS, 16, 128), 2)
    at = lax.broadcasted_iota(jnp.int32, (CHIPS, 16, 128), 1)
    spread = jnp.where(
        lane == at, peak.reshape(CHIPS, 16, 128), jnp.where(lane == at + 16, total.reshape(CHIPS, 16, 128), 0.0)
    )
    return jnp.sum(spread, axis=1)


def wide(tile):
    return jnp.concatenate([tile] * 4, axis=1)


def kernel(
    q_nope, q_rope, w_uk, w_uv, latent, rope, pool, index, lengths, out,
    nope_v, qrope_v, uk_v, uv_v, lat, rop, pool_v, table, index_s, length_s,
    qf, flat, queries, turns, scores, weights, mixed, out_s, in_s, gains,
    out_a, in_a, out_b, in_b, out_t, in_t, att, res,
    load_sem, lat_sem, table_send, table_recv, q_send, q_recv, o_send, o_recv, f_send, f_recv, g_send, g_recv,
    s_send, s_recv, a_send, a_recv, t_send, t_recv, b_send, b_recv,
):
    me = lax.axis_index("tensor")
    core = lax.rem(me, 2)
    chip = me // 2
    row, column = chip // X, lax.rem(chip, X)
    partner = me + 1 - 2 * core

    def peer(j, sign):
        dy, dx = j // X, j % X
        other = lax.rem(row + dy, 2) * X + lax.rem(column + (dx if sign > 0 else X - dx), X)
        return other * 2 + 1 - core

    def remote(src, dst, send, recv, to):
        return pltpu.make_async_remote_copy(
            src_ref=src, dst_ref=dst, send_sem=send, recv_sem=recv,
            device_id={"tensor": to}, device_id_type=MESH,
        )

    def eight(ref, send, recv):
        return remote(ref.at[pl.ds(0, 128)], ref.at[pl.ds(0, 128)], send, recv, partner)

    barrier = pltpu.get_barrier_semaphore()
    for step in range(1, 16):
        pl.semaphore_signal(
            barrier, inc=1, device_id={"tensor": lax.rem(me + step, 16)}, device_id_type=MESH
        )

    small = [
        pltpu.make_async_copy(w_uk, uk_v, load_sem.at[0]),
        pltpu.make_async_copy(q_nope, nope_v, load_sem.at[1]),
        pltpu.make_async_copy(q_rope, qrope_v, load_sem.at[2]),
        pltpu.make_async_copy(pool, pool_v, load_sem.at[3]),
        pltpu.make_async_copy(index, index_s, load_sem.at[4]),
        pltpu.make_async_copy(lengths, length_s, load_sem.at[5]),
    ]
    big = [pltpu.make_async_copy(latent.at[r], lat.at[r], lat_sem.at[r]) for r in range(R)]
    big.insert(1, pltpu.make_async_copy(rope, rop, lat_sem.at[R]))
    late = pltpu.make_async_copy(w_uv, uv_v, load_sem.at[6])
    for copy in small:
        copy.start()
    with jax.named_scope("waitsmall"):
        for copy in small:
            copy.wait()
    own_table = pltpu.make_async_copy(pool_v, table.at[0], load_sem.at[7])
    for copy in [own_table] + big + [late]:
        copy.start()
    qf[...] = nope_v[...].astype(F32).reshape(R * T * H, 128)
    for h in range(H):
        rows = qf[pl.ds(h, R * T, stride=H), :].astype(BF16)
        got = jnp.dot(rows, uk_v[h], preferred_element_type=F32)
        for g in range(4):
            flat[g, pl.ds(h, R * T, stride=H), :] = got[:, 128 * g : 128 * (g + 1)]
    for r in range(R):
        for g in range(4):
            queries[r, 128:144, 128 * g : 128 * (g + 1)] = flat[g, 16 * r : 16 * (r + 1), :].astype(BF16)

    for pair in range(R // 2):
        turned = [qrope_v[2 * pair + n].astype(F32).reshape(16, ROPE) for n in range(2)]
        turns[pair, 128:144] = jnp.concatenate(turned, axis=1).astype(BF16)

    with jax.named_scope("barrier"):
        pl.semaphore_wait(barrier, 15)
    table_copies = [
        remote(pool_v, table.at[step], table_send, table_recv, lax.rem(me + 16 - step, 16))
        for step in (8, 7, 9, 4, 5, 12, 11, 13, 3, 6, 10, 2, 14, 1, 15)
    ]
    for copy in table_copies:
        copy.start()

    q_copies = [
        [
            remote(queries.at[r, pl.ds(128, 16)], queries.at[r, pl.ds(16 * j, 16)],
                   q_send, q_recv.at[r], peer(j, -1))
            for j in ORDER
        ]
        for r in range(R)
    ]
    o_copies = [
        [
            remote(turns.at[p, pl.ds(128, 16)], turns.at[p, pl.ds(16 * j, 16)], o_send, o_recv.at[p], peer(j, -1))
            for j in ORDER
        ]
        for p in range(R // 2)
    ]
    def ask(r):
        for at in range(CHIPS):
            if r % 2 == 0:
                o_copies[r // 2][at].start()
            q_copies[r][at].start()

    ask(0)
    ask(1)
    ask(2)
    ask(3)
    g_copies = [
        remote(turns.at[p, pl.ds(16, 112)], turns.at[p, pl.ds(144, 112)], g_send, g_recv.at[p], partner)
        for p in range(R // 2)
    ]
    f_copies = [
        remote(queries.at[r, pl.ds(16, 112)], queries.at[r, pl.ds(144, 112)],
               f_send, f_recv.at[r], partner)
        for r in range(R)
    ]
    s_copies = [
        remote(out_s.at[r], in_s.at[r], s_send, s_recv.at[r], partner) for r in range(R)
    ]
    a_copies = [
        remote(out_a.at[r], in_a.at[r], a_send, a_recv.at[r], partner) for r in range(R)
    ]
    t_copies = [
        [
            remote(out_t.at[r, pl.ds(j, 1)], in_t.at[r, pl.ds(j, 1)],
                   t_send, t_recv.at[r], peer(j, 1))
            for j in ORDER
        ]
        for r in range(R)
    ]
    b_copies = [
        [
            remote(out_b.at[r, pl.ds(16 * j, 16)], in_b.at[r, pl.ds(16 * j, 16)],
                   b_send, b_recv.at[r], peer(j, 1))
            for j in ORDER
        ]
        for r in range(R)
    ]

    def forward(r):
        if r % 2 == 0:
            eight(turns.at[r // 2], o_send, o_recv.at[r // 2]).wait_recv()
            g_copies[r // 2].start()
        eight(queries.at[r], q_send, q_recv.at[r]).wait_recv()
        f_copies[r].start()

    def forwarded(r):
        if r % 2 == 0:
            g_copies[r // 2].wait_recv()
        f_copies[r].wait_recv()

    with jax.named_scope("waittable"):
        remote(table.at[pl.ds(1, 15)], table.at[pl.ds(1, 15)], table_send, table_recv, partner).wait_recv()
        own_table.wait()

    def scale_block(r, b):
        at = index_s[r, b]
        slot = lax.rem(at // 64 + 16 - me, 16)
        col = lax.rem(at, 64)
        rows = pl.ds(pl.multiple_of(b * 128, 128), 128)
        for g in range(4):
            lat[r, rows, 128 * g : 128 * (g + 1)] = (
                lat[r, rows, 128 * g : 128 * (g + 1)].astype(F32) * table[slot, g, col]
            ).astype(BF16)
        rop[r, :, rows] = (rop[r, :, rows].astype(F32) * table[slot, 4, col]).astype(BF16)

    def scale(r, first=0, last=BLOCKS):
        if first == 0 and last > 0:
            big[r + 1 if r else 0].wait()
            if r == 0:
                big[1].wait()

        def one(b, carry):
            scale_block(r, b)
            return carry

        lax.fori_loop(first, last, one, 0, unroll=SCALE_UNROLL)

    def score(r, n, top):
        cols = pl.ds(n * WIDTH, WIDTH)
        got = lax.dot_general(
            queries[r], lat[r, cols, :], (((1,), (1,)), ((), ())),
            preferred_element_type=F32,
        ) + jnp.dot(
            turns[r // 2, :, ROPE * (r % 2) : ROPE * (r % 2 + 1)], rop[r, :, cols], preferred_element_type=F32
        )
        place = lax.broadcasted_iota(jnp.int32, (1, T, 8, WIDTH), 3) + (me * SPAN + n * WIDTH)
        limit = length_s[r] - T + lax.broadcasted_iota(jnp.int32, (1, T, 8, WIDTH), 1)
        got = jnp.where(place <= limit, got.reshape(16, T, 8, WIDTH), MASKED).reshape(ROWS, WIDTH)
        scores[r % 2, :, cols] = got
        for g in range(WIDTH // 128):
            top = jnp.maximum(top, got[:, 128 * g : 128 * (g + 1)])
        return top

    def weigh(r, n, peak, total, rows=slice(0, ROWS)):
        cols = pl.ds(n * WIDTH, WIDTH)
        got = jnp.exp2((scores[r % 2, rows, cols] - peak[rows]) * FACTOR)
        weights[rows, cols] = got.astype(BF16)
        for g in range(WIDTH // 128):
            total = total + got[:, 128 * g : 128 * (g + 1)]
        return total

    def look(r, between=None):
        top = jnp.full((ROWS, 128), -3e38, F32)
        for n in range(CHUNKS):
            if between is not None and n == between[0]:
                between[1]()
            top = score(r, n, top)
        return jnp.max(top, axis=1, keepdims=True)

    def tell(r, peak, total):
        peak_w = jnp.broadcast_to(peak, (ROWS, 128))
        total_w = jnp.broadcast_to(total, (ROWS, 128))
        out_s[r, :, 0:128] = peak_w[128:]
        out_s[r, :, 128:256] = total_w[128:]
        s_copies[r].start()
        gains[r, :, 0:128] = peak_w[:128]
        gains[r, :, 128:256] = total_w[:128]

    def keep(r, got):
        out_a[r] = got[128:].astype(BF16)
        a_copies[r].start()
        mixed[r] = got[:128]

    def factors_of(r):
        peak_0, total_0 = gains[r, :, 0:128], gains[r, :, 128:256]
        peak_1, total_1 = in_s[r, :, 0:128], in_s[r, :, 128:256]
        peak = jnp.maximum(peak_0, peak_1)
        gain_0 = jnp.exp2((peak_0 - peak) * FACTOR)
        gain_1 = jnp.exp2((peak_1 - peak) * FACTOR)
        out_t[r] = stats_rows(peak, total_0 * gain_0 + total_1 * gain_1)
        return gain_0, gain_1

    def join(r, gain_0, gain_1):
        out_b[r] = (mixed[r] * wide(gain_0) + in_a[r].astype(F32) * wide(gain_1)).astype(BF16)

    def combine(r):
        with jax.named_scope(f"waits{r}"):
            s_copies[r].wait_recv()
        both_gains = factors_of(r)
        for copy in t_copies[r]:
            copy.start()
        with jax.named_scope(f"waita{r}"):
            a_copies[r].wait_recv()
        join(r, *both_gains)
        for copy in b_copies[r]:
            copy.start()

    def mix_last(r, peak):
        with jax.named_scope(f"waitsa{r-1}"):
            s_copies[r - 1].wait_recv()
            a_copies[r - 1].wait_recv()
        with jax.named_scope(f"mix{r}"):
            join(r - 1, *factors_of(r - 1))
            peak_w = jnp.broadcast_to(peak, (ROWS, 128))
            for rows in (slice(128, 256), slice(0, 128)):
                total, got = jnp.zeros((128, 128), F32), None
                for n in range(CHUNKS):
                    total = weigh(r, n, peak, total, rows)
                got = jnp.dot(weights[rows], lat[r], preferred_element_type=F32)
                total_w = jnp.broadcast_to(jnp.sum(total, axis=1, keepdims=True), (128, 128))
                if rows.start:
                    out_s[r, :, 0:128] = peak_w[128:]
                    out_s[r, :, 128:256] = total_w
                    s_copies[r].start()
                    out_a[r] = got.astype(BF16)
                    a_copies[r].start()
                    for copy in t_copies[r - 1] + b_copies[r - 1]:
                        copy.start()
                else:
                    gains[r, :, 0:128] = peak_w[:128]
                    gains[r, :, 128:256] = total_w
                    mixed[r] = got

    def mix(r, peak):
        if r >= 1 and MERGE:
            with jax.named_scope(f"waitsa{r-1}"):
                s_copies[r - 1].wait_recv()
                a_copies[r - 1].wait_recv()
        elif r >= 1:
            combine(r - 1)
        with jax.named_scope(f"mix{r}"):
            total, got = jnp.zeros((ROWS, 128), F32), None
            for n in range(CHUNKS):
                total = weigh(r, n, peak, total)
            if r >= 1 and MERGE:
                join(r - 1, *factors_of(r - 1))
            for n in range(CHUNKS):
                cols = pl.ds(n * WIDTH, WIDTH)
                one = jnp.dot(weights[:, cols], lat[r, cols, :], preferred_element_type=F32)
                got = one if got is None else got + one
            if r >= 1 and MERGE:
                for copy in t_copies[r - 1] + b_copies[r - 1]:
                    copy.start()
            tell(r, peak, jnp.sum(total, axis=1, keepdims=True))
            keep(r, got)

    def finish(r):
        with jax.named_scope(f"waitt{r}"):
            remote(out_t.at[r], in_t.at[r], t_send, t_recv.at[r], partner).wait_recv()
        found = in_t[r]
        factors = jnp.exp2((found - jnp.max(found, axis=0, keepdims=True)) * FACTOR)
        total = jnp.sum(factors * pltpu.roll(found, 112, 1), axis=0, keepdims=True)
        lane = lax.broadcasted_iota(jnp.int32, (CHIPS, 128), 1)
        factors = jnp.transpose(jnp.where(lane < 16, factors / total, 0.0))[0:16]
        factors = [jnp.broadcast_to(factors[:, j : j + 1], (16, LAT)) for j in range(CHIPS)]
        with jax.named_scope(f"waitb{r}"):
            eight(in_b.at[r], b_send, b_recv.at[r]).wait_recv()
        attended = jnp.zeros((16, LAT), F32)
        for j in range(CHIPS):
            attended = attended + in_b[r, 16 * j : 16 * (j + 1)].astype(F32) * factors[j]
        for g in range(4):
            att[g, 16 * r : 16 * (r + 1), :] = attended[:, 128 * g : 128 * (g + 1)]

    with jax.named_scope("scale0"):
        scale(0)
    with jax.named_scope("scale1"):
        scale(1, 0, 8)
    with jax.named_scope("forward0"):
        forward(0)
    with jax.named_scope("scale2"):
        scale(1, 8, 16)
        scale(2)
    scale(3, 0, SPLIT)
    for r in range(R):
        with jax.named_scope(f"waitf{r}"):
            if 1 <= r < R - 1:
                forward(r + 1)
            forwarded(r)
        with jax.named_scope(f"score{r}"):
            peak = look(r, (1, functools.partial(forward, 1)) if r == 0 else None)
        if r == 0:
            with jax.named_scope("scale3"):
                scale(3, SPLIT, BLOCKS)
        mix_last(r, peak) if r == R - 1 else mix(r, peak)
    combine(R - 1)
    for r in range(R):
        finish(r)

    late.wait()
    for h in range(H):
        rows = jnp.concatenate(
            [att[g, pl.ds(h, R * T, stride=H), :] for g in range(4)], axis=1
        ).astype(BF16)
        res[pl.ds(h, R * T, stride=H), :] = jnp.dot(rows, uv_v[h], preferred_element_type=F32)
    out[...] = res[...].reshape(R, T, H, 128).astype(BF16)

    with jax.named_scope("drain"):
        remote(table.at[pl.ds(1, 15)], table.at[pl.ds(1, 15)], table_send, table_recv, partner).wait_send()
        for ref, rows, send in (
            (queries, pl.ds(0, 128), q_send), (turns, pl.ds(0, 128), o_send), (turns, pl.ds(16, 112), g_send),
            (queries, pl.ds(16, 112), f_send), (out_s, pl.ds(0, 128), s_send),
            (out_a, pl.ds(0, 128), a_send), (out_t, pl.ds(0, 8), t_send), (out_b, pl.ds(0, 128), b_send),
        ):
            remote(ref.at[:, rows], ref.at[:, rows], send, table_recv, partner).wait_send()


def local(*args):
    dma = pltpu.SemaphoreType.DMA
    return pl.pallas_call(
        kernel,
        out_shape=pltpu.VMEM((R, T, H, 128), BF16),
        in_specs=[pl.BlockSpec(memory_space=pl.ANY)] * 9,
        out_specs=pl.BlockSpec(memory_space=pltpu.VMEM),
        scratch_shapes=[
            pltpu.VMEM((R, T, H, 128), BF16),
            pltpu.VMEM((R, T, H, ROPE), BF16),
            pltpu.VMEM((H, 128, LAT), BF16),
            pltpu.VMEM((H, LAT, 128), BF16),
            pltpu.VMEM((R, SPAN, LAT), BF16),
            pltpu.VMEM((R, ROPE, SPAN), BF16),
            pltpu.VMEM((5, 64), F32),
            pltpu.SMEM((16, 5, 64), F32),
            pltpu.SMEM((R, BLOCKS), jnp.int32),
            pltpu.SMEM((R,), jnp.int32),
            pltpu.VMEM((R * T * H, 128), F32),
            pltpu.VMEM((4, R * T * H, 128), F32),
            pltpu.VMEM((R, ROWS, LAT), BF16),
            pltpu.VMEM((R // 2, ROWS, 128), BF16),
            pltpu.VMEM((2, ROWS, SPAN), F32),
            pltpu.VMEM((ROWS, SPAN), BF16),
            pltpu.VMEM((R, 128, LAT), F32),
            pltpu.VMEM((R, 128, 256), F32),
            pltpu.VMEM((R, 128, 256), F32),
            pltpu.VMEM((R, 128, 256), F32),
            pltpu.VMEM((R, 128, LAT), BF16),
            pltpu.VMEM((R, 128, LAT), BF16),
            pltpu.VMEM((R, 128, LAT), BF16),
            pltpu.VMEM((R, 128, LAT), BF16),
            pltpu.VMEM((R, CHIPS, 128), F32),
            pltpu.VMEM((R, CHIPS, 128), F32),
            pltpu.VMEM((4, R * T * H, 128), F32),
            pltpu.VMEM((R * T * H, 128), F32),
            dma((8,)),
            dma((R + 1,)),
            dma(()),
            dma(()),
            dma(()),
            dma((R,)),
            dma(()),
            dma((R // 2,)),
            dma(()),
            dma((R,)),
            dma(()),
            dma((R // 2,)),
            dma(()),
            dma((R,)),
            dma(()),
            dma((R,)),
            dma(()),
            dma((R,)),
            dma(()),
            dma((R,)),
        ],
        compiler_params=pltpu.CompilerParams(collective_id=0, has_side_effects=True),
        name="decode",
    )(*args)


def solution(mesh):
    placed = (
        P("dp", None, "tensor", None),
        P("dp", None, "tensor", None),
        P("tensor", None, None),
        P("tensor", None, None),
        P("dp", "tensor", None),
        P("dp", None, "tensor"),
        P(None, ("dp", "tensor")),
        P("dp", "tensor"),
        P("dp"),
    )
    return jax.shard_map(
        local, mesh=mesh, in_specs=placed, out_specs=P("dp", None, "tensor", None), check_vma=False
    )
```

```python
import functools
import math

import jax
import jax.numpy as jnp
from jax import lax
from jax.experimental import pallas as pl
from jax.experimental.pallas import tpu as pltpu
from jax.sharding import PartitionSpec as P

MESH = pl.DeviceIdType.MESH
R, T, H = 4, 2, 8
ROWS, LAT, ROPE = 256, 512, 64
SPAN, BLOCKS = 2048, 16
X, CHIPS = 4, 8
FACTOR = (128 + 64) ** -0.5 * math.log2(math.e)
MASKED = -1e30
MERGE = True
SPLIT = 8
SCALE_UNROLL = 4
F32, BF16 = jnp.float32, jnp.bfloat16


ORDER = (6, 2, 5, 7, 1, 3, 4, 0)
WIDTH = 512
CHUNKS = SPAN // WIDTH


def stats_rows(peak, total):
    lane = lax.broadcasted_iota(jnp.int32, (CHIPS, 16, 128), 2)
    at = lax.broadcasted_iota(jnp.int32, (CHIPS, 16, 128), 1)
    spread = jnp.where(
        lane == at, peak.reshape(CHIPS, 16, 128), jnp.where(lane == at + 16, total.reshape(CHIPS, 16, 128), 0.0)
    )
    return jnp.sum(spread, axis=1)


def wide(tile):
    return jnp.concatenate([tile] * 4, axis=1)


def kernel(
    q_nope, q_rope, w_uk, w_uv, latent, rope, pool, index, lengths, out,
    nope_v, qrope_v, uk_v, uv_v, lat, rop, pool_v, table, index_s, length_s,
    qf, flat, queries, turns, scores, weights, mixed, out_s, in_s, gains,
    out_a, in_a, out_b, in_b, out_t, in_t, att, res,
    load_sem, lat_sem, table_send, table_recv, q_send, q_recv, o_send, o_recv, f_send, f_recv, g_send, g_recv,
    s_send, s_recv, a_send, a_recv, t_send, t_recv, b_send, b_recv,
):
    me = lax.axis_index("tensor")
    core = lax.rem(me, 2)
    chip = me // 2
    row, column = chip // X, lax.rem(chip, X)
    partner = me + 1 - 2 * core

    def peer(j, sign):
        dy, dx = j // X, j % X
        other = lax.rem(row + dy, 2) * X + lax.rem(column + (dx if sign > 0 else X - dx), X)
        return other * 2 + 1 - core

    def remote(src, dst, send, recv, to):
        return pltpu.make_async_remote_copy(
            src_ref=src, dst_ref=dst, send_sem=send, recv_sem=recv,
            device_id={"tensor": to}, device_id_type=MESH,
        )

    def eight(ref, send, recv):
        return remote(ref.at[pl.ds(0, 128)], ref.at[pl.ds(0, 128)], send, recv, partner)

    barrier = pltpu.get_barrier_semaphore()
    for step in range(1, 16):
        pl.semaphore_signal(
            barrier, inc=1, device_id={"tensor": lax.rem(me + step, 16)}, device_id_type=MESH
        )

    small = [
        pltpu.make_async_copy(w_uk, uk_v, load_sem.at[0]),
        pltpu.make_async_copy(q_nope, nope_v, load_sem.at[1]),
        pltpu.make_async_copy(q_rope, qrope_v, load_sem.at[2]),
        pltpu.make_async_copy(pool, pool_v, load_sem.at[3]),
        pltpu.make_async_copy(index, index_s, load_sem.at[4]),
        pltpu.make_async_copy(lengths, length_s, load_sem.at[5]),
    ]
    big = [pltpu.make_async_copy(latent.at[r], lat.at[r], lat_sem.at[r]) for r in range(R)]
    big.insert(1, pltpu.make_async_copy(rope, rop, lat_sem.at[R]))
    late = pltpu.make_async_copy(w_uv, uv_v, load_sem.at[6])
    for copy in small:
        copy.start()
    with jax.named_scope("waitsmall"):
        for copy in small:
            copy.wait()
    own_table = pltpu.make_async_copy(pool_v, table.at[0], load_sem.at[7])
    for copy in [own_table] + big + [late]:
        copy.start()
    qf[...] = nope_v[...].astype(F32).reshape(R * T * H, 128)
    for h in range(H):
        rows = qf[pl.ds(h, R * T, stride=H), :].astype(BF16)
        got = jnp.dot(rows, uk_v[h], preferred_element_type=F32)
        for g in range(4):
            flat[g, pl.ds(h, R * T, stride=H), :] = got[:, 128 * g : 128 * (g + 1)]
    for r in range(R):
        for g in range(4):
            queries[r, 128:144, 128 * g : 128 * (g + 1)] = flat[g, 16 * r : 16 * (r + 1), :].astype(BF16)

    for pair in range(R // 2):
        turned = [qrope_v[2 * pair + n].astype(F32).reshape(16, ROPE) for n in range(2)]
        turns[pair, 128:144] = jnp.concatenate(turned, axis=1).astype(BF16)

    with jax.named_scope("barrier"):
        pl.semaphore_wait(barrier, 15)
    table_copies = [
        remote(pool_v, table.at[step], table_send, table_recv, lax.rem(me + 16 - step, 16))
        for step in (8, 7, 9, 4, 5, 12, 11, 13, 3, 6, 10, 2, 14, 1, 15)
    ]
    for copy in table_copies:
        copy.start()

    q_copies = [
        [
            remote(queries.at[r, pl.ds(128, 16)], queries.at[r, pl.ds(16 * j, 16)],
                   q_send, q_recv.at[r], peer(j, -1))
            for j in ORDER
        ]
        for r in range(R)
    ]
    o_copies = [
        [
            remote(turns.at[p, pl.ds(128, 16)], turns.at[p, pl.ds(16 * j, 16)], o_send, o_recv.at[p], peer(j, -1))
            for j in ORDER
        ]
        for p in range(R // 2)
    ]
    def ask(r):
        for at in range(CHIPS):
            if r % 2 == 0:
                o_copies[r // 2][at].start()
            q_copies[r][at].start()

    ask(0)
    ask(1)
    ask(2)
    ask(3)
    g_copies = [
        remote(turns.at[p, pl.ds(16, 112)], turns.at[p, pl.ds(144, 112)], g_send, g_recv.at[p], partner)
        for p in range(R // 2)
    ]
    f_copies = [
        remote(queries.at[r, pl.ds(16, 112)], queries.at[r, pl.ds(144, 112)],
               f_send, f_recv.at[r], partner)
        for r in range(R)
    ]
    s_copies = [
        remote(out_s.at[r], in_s.at[r], s_send, s_recv.at[r], partner) for r in range(R)
    ]
    a_copies = [
        remote(out_a.at[r], in_a.at[r], a_send, a_recv.at[r], partner) for r in range(R)
    ]
    t_copies = [
        [
            remote(out_t.at[r, pl.ds(j, 1)], in_t.at[r, pl.ds(j, 1)],
                   t_send, t_recv.at[r], peer(j, 1))
            for j in ORDER
        ]
        for r in range(R)
    ]
    b_copies = [
        [
            remote(out_b.at[r, pl.ds(16 * j, 16)], in_b.at[r, pl.ds(16 * j, 16)],
                   b_send, b_recv.at[r], peer(j, 1))
            for j in ORDER
        ]
        for r in range(R)
    ]

    def forward(r):
        if r % 2 == 0:
            eight(turns.at[r // 2], o_send, o_recv.at[r // 2]).wait_recv()
            g_copies[r // 2].start()
        eight(queries.at[r], q_send, q_recv.at[r]).wait_recv()
        f_copies[r].start()

    def forwarded(r):
        if r % 2 == 0:
            g_copies[r // 2].wait_recv()
        f_copies[r].wait_recv()

    with jax.named_scope("waittable"):
        remote(table.at[pl.ds(1, 15)], table.at[pl.ds(1, 15)], table_send, table_recv, partner).wait_recv()
        own_table.wait()

    def scale_block(r, b):
        at = index_s[r, b]
        slot = lax.rem(at // 64 + 16 - me, 16)
        col = lax.rem(at, 64)
        rows = pl.ds(pl.multiple_of(b * 128, 128), 128)
        for g in range(4):
            lat[r, rows, 128 * g : 128 * (g + 1)] = (
                lat[r, rows, 128 * g : 128 * (g + 1)].astype(F32) * table[slot, g, col]
            ).astype(BF16)
        rop[r, :, rows] = (rop[r, :, rows].astype(F32) * table[slot, 4, col]).astype(BF16)

    def scale(r, first=0, last=BLOCKS):
        if first == 0 and last > 0:
            big[r + 1 if r else 0].wait()
            if r == 0:
                big[1].wait()

        def one(b, carry):
            scale_block(r, b)
            return carry

        lax.fori_loop(first, last, one, 0, unroll=SCALE_UNROLL)

    def score(r, n, top):
        cols = pl.ds(n * WIDTH, WIDTH)
        got = lax.dot_general(
            queries[r], lat[r, cols, :], (((1,), (1,)), ((), ())),
            preferred_element_type=F32,
        ) + jnp.dot(
            turns[r // 2, :, ROPE * (r % 2) : ROPE * (r % 2 + 1)], rop[r, :, cols], preferred_element_type=F32
        )
        place = lax.broadcasted_iota(jnp.int32, (1, T, 8, WIDTH), 3) + (me * SPAN + n * WIDTH)
        limit = length_s[r] - T + lax.broadcasted_iota(jnp.int32, (1, T, 8, WIDTH), 1)
        got = jnp.where(place <= limit, got.reshape(16, T, 8, WIDTH), MASKED).reshape(ROWS, WIDTH)
        scores[r % 2, :, cols] = got
        for g in range(WIDTH // 128):
            top = jnp.maximum(top, got[:, 128 * g : 128 * (g + 1)])
        return top

    def weigh(r, n, peak, total, rows=slice(0, ROWS)):
        cols = pl.ds(n * WIDTH, WIDTH)
        got = jnp.exp2((scores[r % 2, rows, cols] - peak[rows]) * FACTOR)
        weights[rows, cols] = got.astype(BF16)
        for g in range(WIDTH // 128):
            total = total + got[:, 128 * g : 128 * (g + 1)]
        return total

    def look(r, between=None):
        top = jnp.full((ROWS, 128), -3e38, F32)
        for n in range(CHUNKS):
            if between is not None and n == between[0]:
                between[1]()
            top = score(r, n, top)
        return jnp.max(top, axis=1, keepdims=True)

    def tell(r, peak, total):
        peak_w = jnp.broadcast_to(peak, (ROWS, 128))
        total_w = jnp.broadcast_to(total, (ROWS, 128))
        out_s[r, :, 0:128] = peak_w[128:]
        out_s[r, :, 128:256] = total_w[128:]
        s_copies[r].start()
        gains[r, :, 0:128] = peak_w[:128]
        gains[r, :, 128:256] = total_w[:128]

    def keep(r, got):
        out_a[r] = got[128:].astype(BF16)
        a_copies[r].start()
        mixed[r] = got[:128]

    def factors_of(r):
        peak_0, total_0 = gains[r, :, 0:128], gains[r, :, 128:256]
        peak_1, total_1 = in_s[r, :, 0:128], in_s[r, :, 128:256]
        peak = jnp.maximum(peak_0, peak_1)
        gain_0 = jnp.exp2((peak_0 - peak) * FACTOR)
        gain_1 = jnp.exp2((peak_1 - peak) * FACTOR)
        out_t[r] = stats_rows(peak, total_0 * gain_0 + total_1 * gain_1)
        return gain_0, gain_1

    def join(r, gain_0, gain_1):
        out_b[r] = (mixed[r] * wide(gain_0) + in_a[r].astype(F32) * wide(gain_1)).astype(BF16)

    def combine(r):
        with jax.named_scope(f"waits{r}"):
            s_copies[r].wait_recv()
        both_gains = factors_of(r)
        for copy in t_copies[r]:
            copy.start()
        with jax.named_scope(f"waita{r}"):
            a_copies[r].wait_recv()
        gain_0, gain_1 = both_gains
        for j, copy in zip(ORDER, b_copies[r]):
            rows = slice(16 * j, 16 * (j + 1))
            out_b[r, rows] = (
                mixed[r, rows] * wide(gain_0[rows]) + in_a[r, rows].astype(F32) * wide(gain_1[rows])
            ).astype(BF16)
            copy.start()

    def mix_last(r, peak):
        with jax.named_scope(f"waitsa{r-1}"):
            s_copies[r - 1].wait_recv()
            a_copies[r - 1].wait_recv()
        with jax.named_scope(f"mix{r}"):
            join(r - 1, *factors_of(r - 1))
            peak_w = jnp.broadcast_to(peak, (ROWS, 128))
            for rows in (slice(128, 256), slice(0, 128)):
                total, got = jnp.zeros((128, 128), F32), None
                for n in range(CHUNKS):
                    total = weigh(r, n, peak, total, rows)
                got = jnp.dot(weights[rows], lat[r], preferred_element_type=F32)
                total_w = jnp.broadcast_to(jnp.sum(total, axis=1, keepdims=True), (128, 128))
                if rows.start:
                    out_s[r, :, 0:128] = peak_w[128:]
                    out_s[r, :, 128:256] = total_w
                    s_copies[r].start()
                    out_a[r] = got.astype(BF16)
                    a_copies[r].start()
                    for copy in t_copies[r - 1] + b_copies[r - 1]:
                        copy.start()
                else:
                    gains[r, :, 0:128] = peak_w[:128]
                    gains[r, :, 128:256] = total_w
                    mixed[r] = got

    def mix(r, peak):
        if r >= 1 and MERGE:
            with jax.named_scope(f"waitsa{r-1}"):
                s_copies[r - 1].wait_recv()
                a_copies[r - 1].wait_recv()
        elif r >= 1:
            combine(r - 1)
        with jax.named_scope(f"mix{r}"):
            total, got = jnp.zeros((ROWS, 128), F32), None
            for n in range(CHUNKS):
                total = weigh(r, n, peak, total)
            if r >= 1 and MERGE:
                join(r - 1, *factors_of(r - 1))
            for n in range(CHUNKS):
                cols = pl.ds(n * WIDTH, WIDTH)
                one = jnp.dot(weights[:, cols], lat[r, cols, :], preferred_element_type=F32)
                got = one if got is None else got + one
            if r >= 1 and MERGE:
                for copy in t_copies[r - 1] + b_copies[r - 1]:
                    copy.start()
            tell(r, peak, jnp.sum(total, axis=1, keepdims=True))
            keep(r, got)

    def finish(r):
        with jax.named_scope(f"waitt{r}"):
            remote(out_t.at[r], in_t.at[r], t_send, t_recv.at[r], partner).wait_recv()
        found = in_t[r]
        factors = jnp.exp2((found - jnp.max(found, axis=0, keepdims=True)) * FACTOR)
        total = jnp.sum(factors * pltpu.roll(found, 112, 1), axis=0, keepdims=True)
        lane = lax.broadcasted_iota(jnp.int32, (CHIPS, 128), 1)
        factors = jnp.transpose(jnp.where(lane < 16, factors / total, 0.0))[0:16]
        factors = [jnp.broadcast_to(factors[:, j : j + 1], (16, LAT)) for j in range(CHIPS)]
        with jax.named_scope(f"waitb{r}"):
            eight(in_b.at[r], b_send, b_recv.at[r]).wait_recv()
        attended = jnp.zeros((16, LAT), F32)
        for j in range(CHIPS):
            attended = attended + in_b[r, 16 * j : 16 * (j + 1)].astype(F32) * factors[j]
        for g in range(4):
            att[g, 16 * r : 16 * (r + 1), :] = attended[:, 128 * g : 128 * (g + 1)]

    with jax.named_scope("scale0"):
        scale(0)
    with jax.named_scope("scale1"):
        scale(1, 0, 8)
    with jax.named_scope("forward0"):
        forward(0)
    with jax.named_scope("scale2"):
        scale(1, 8, 16)
        scale(2)
    scale(3, 0, SPLIT)
    for r in range(R):
        with jax.named_scope(f"waitf{r}"):
            if 1 <= r < R - 1:
                forward(r + 1)
            forwarded(r)
        with jax.named_scope(f"score{r}"):
            peak = look(r, (1, functools.partial(forward, 1)) if r == 0 else None)
        if r == 0:
            with jax.named_scope("scale3"):
                scale(3, SPLIT, BLOCKS)
        mix_last(r, peak) if r == R - 1 else mix(r, peak)
    combine(R - 1)
    for r in range(R):
        finish(r)

    late.wait()
    for h in range(H):
        rows = jnp.concatenate(
            [att[g, pl.ds(h, R * T, stride=H), :] for g in range(4)], axis=1
        ).astype(BF16)
        res[pl.ds(h, R * T, stride=H), :] = jnp.dot(rows, uv_v[h], preferred_element_type=F32)
    out[...] = res[...].reshape(R, T, H, 128).astype(BF16)

    with jax.named_scope("drain"):
        remote(table.at[pl.ds(1, 15)], table.at[pl.ds(1, 15)], table_send, table_recv, partner).wait_send()
        for ref, rows, send in (
            (queries, pl.ds(0, 128), q_send), (turns, pl.ds(0, 128), o_send), (turns, pl.ds(16, 112), g_send),
            (queries, pl.ds(16, 112), f_send), (out_s, pl.ds(0, 128), s_send),
            (out_a, pl.ds(0, 128), a_send), (out_t, pl.ds(0, 8), t_send), (out_b, pl.ds(0, 128), b_send),
        ):
            remote(ref.at[:, rows], ref.at[:, rows], send, table_recv, partner).wait_send()


def local(*args):
    dma = pltpu.SemaphoreType.DMA
    return pl.pallas_call(
        kernel,
        out_shape=pltpu.VMEM((R, T, H, 128), BF16),
        in_specs=[pl.BlockSpec(memory_space=pl.ANY)] * 9,
        out_specs=pl.BlockSpec(memory_space=pltpu.VMEM),
        scratch_shapes=[
            pltpu.VMEM((R, T, H, 128), BF16),
            pltpu.VMEM((R, T, H, ROPE), BF16),
            pltpu.VMEM((H, 128, LAT), BF16),
            pltpu.VMEM((H, LAT, 128), BF16),
            pltpu.VMEM((R, SPAN, LAT), BF16),
            pltpu.VMEM((R, ROPE, SPAN), BF16),
            pltpu.VMEM((5, 64), F32),
            pltpu.SMEM((16, 5, 64), F32),
            pltpu.SMEM((R, BLOCKS), jnp.int32),
            pltpu.SMEM((R,), jnp.int32),
            pltpu.VMEM((R * T * H, 128), F32),
            pltpu.VMEM((4, R * T * H, 128), F32),
            pltpu.VMEM((R, ROWS, LAT), BF16),
            pltpu.VMEM((R // 2, ROWS, 128), BF16),
            pltpu.VMEM((2, ROWS, SPAN), F32),
            pltpu.VMEM((ROWS, SPAN), BF16),
            pltpu.VMEM((R, 128, LAT), F32),
            pltpu.VMEM((R, 128, 256), F32),
            pltpu.VMEM((R, 128, 256), F32),
            pltpu.VMEM((R, 128, 256), F32),
            pltpu.VMEM((R, 128, LAT), BF16),
            pltpu.VMEM((R, 128, LAT), BF16),
            pltpu.VMEM((R, 128, LAT), BF16),
            pltpu.VMEM((R, 128, LAT), BF16),
            pltpu.VMEM((R, CHIPS, 128), F32),
            pltpu.VMEM((R, CHIPS, 128), F32),
            pltpu.VMEM((4, R * T * H, 128), F32),
            pltpu.VMEM((R * T * H, 128), F32),
            dma((8,)),
            dma((R + 1,)),
            dma(()),
            dma(()),
            dma(()),
            dma((R,)),
            dma(()),
            dma((R // 2,)),
            dma(()),
            dma((R,)),
            dma(()),
            dma((R // 2,)),
            dma(()),
            dma((R,)),
            dma(()),
            dma((R,)),
            dma(()),
            dma((R,)),
            dma(()),
            dma((R,)),
        ],
        compiler_params=pltpu.CompilerParams(collective_id=0, has_side_effects=True),
        name="decode",
    )(*args)


def solution(mesh):
    placed = (
        P("dp", None, "tensor", None),
        P("dp", None, "tensor", None),
        P("tensor", None, None),
        P("tensor", None, None),
        P("dp", "tensor", None),
        P("dp", None, "tensor"),
        P(None, ("dp", "tensor")),
        P("dp", "tensor"),
        P("dp"),
    )
    return jax.shard_map(
        local, mesh=mesh, in_specs=placed, out_specs=P("dp", None, "tensor", None), check_vma=False
    )
```
